32 devices in a mesh: gx: 2 (over x), gy: 4 (over y, core), gz: 4 (over z).
Axes of the slice: x: 2, y: 2, z: 4, core: 2. Of those that a mesh axis runs over, the one named last changes fastest.
Arguments:
- vorticity: float32 [3, 16, 64, 512], P(None, 'gx', 'gy', 'gz'), may hold values from -6 to 6
- velocity: float32 [3, 16, 64, 512], P(None, 'gx', 'gy', 'gz'), may hold values from -1 to 1
Outputs:
- vorticity_out: float32 [3, 16, 64, 512], P(None, 'gx', 'gy', 'gz')
The draws below stay inside these ranges and needn't reach their ends.
All inputs are finite; a program needn't handle non-finite values.
Results may differ from the reference program's by a relative error of at most 0.0003.
Values sent between devices are 32-bit elements; how exact they have to be, the bound alone decides.
A program may use at most 64 MiB of HBM per device.

```python
import jax
import jax.numpy as jnp

SUBSTEPS = 2
NX = 16
NY = 64
NZ = 512


def level_of(key, shape, shards, least, largest):
    def one(position, blocks):
        heights = jax.random.uniform(jax.random.fold_in(jax.random.fold_in(key, 6), position), (blocks,), jnp.float32, least / len(shards), largest / len(shards))
        return jnp.repeat(jnp.exp(heights), shape[position] // blocks).reshape((-1,) + (1,) * (len(shape) - position - 1))

    gain = one(*shards[0])
    for cut in shards[1:]:
        gain = gain * one(*cut)
    return gain


def bell_draw(stream_key, extent, deviation, bound, split=(), held_as=jnp.bfloat16):
    factor_of = level_of(stream_key, extent, split, -0.22, 0.18) if split else 1.0
    array = jax.random.normal(stream_key, extent, jnp.float32) * deviation * factor_of
    return jnp.minimum(jnp.maximum(array, -bound), bound).astype(held_as)


def setup_inputs(seed: int = 0) -> dict:
    splits = jax.random.split(jax.random.key(seed), 3)
    vorticity = bell_draw(splits[0], (3, NX, NY, NZ), 1.0, 6.0, ((1, 2), (2, 4), (3, 4)), jnp.float32)
    velocity = jnp.clip(jax.random.uniform(splits[1], (3, NX, NY, NZ), jnp.float32, -1.0, 1.0) * level_of(splits[1], (3, NX, NY, NZ), ((1, 2), (2, 4), (3, 4)), -0.4, 0.0), -1.0, 1.0)
    return dict(vorticity=vorticity, velocity=velocity)


time_step = 0.5


def kernel(distance):
    magnitude = jnp.abs(distance)
    near = 1.0 - 2.5 * magnitude * magnitude + 1.5 * magnitude * magnitude * magnitude
    far = 0.5 * (2.0 - magnitude) * (2.0 - magnitude) * (1.0 - magnitude)
    return jnp.where(magnitude < 1.0, near, jnp.where(magnitude < 2.0, far, 0.0))


def remesh(current, displace, along):
    total = jnp.zeros_like(current)
    for offset in range(-2, 3):
        total = total + jnp.roll(kernel(offset - displace) * current, offset, axis=along)
    return total


def derive(values, along):
    near_diff = jnp.roll(values, -1, axis=along) - jnp.roll(values, 1, axis=along)
    far_diff = jnp.roll(values, -2, axis=along) - jnp.roll(values, 2, axis=along)
    return (8.0 * near_diff - far_diff) / 12.0


def reference(vorticity, velocity):
    slopes = [derive(velocity, along) for along in (1, 2, 3)]
    current = vorticity
    for substep in range(SUBSTEPS):
        for along in (1, 2, 3):
            current = remesh(current, time_step * velocity[along - 1], along)
        stretch = current[0] * slopes[0] + current[1] * slopes[1] + current[2] * slopes[2]
        current = current + time_step * stretch
    return current
```

```python
import functools

import jax
import jax.numpy as jnp
from jax import lax
from jax.experimental import pallas as pl
from jax.experimental.pallas import tpu as pltpu
from jax.sharding import PartitionSpec as P

SUBSTEPS = 2
TIME_STEP = 0.5
AXES = ("gx", "gy", "gz")
MESH = pl.DeviceIdType.MESH


def roll(values, shift, axis):
    return pltpu.roll(values, shift % values.shape[axis], axis)


def weights(velocity):
    d = TIME_STEP * velocity
    s = jnp.abs(d)
    t = 1.0 - s
    positive = d > 0.0
    centre = 1.0 + s * s * (1.5 * s - 2.5)
    toward = 1.0 + t * t * (1.5 * t - 2.5)
    away = -0.5 * s * t * t
    beyond = -0.5 * s * s * t
    return (
        jnp.where(positive, 0.0, beyond),
        jnp.where(positive, away, toward),
        centre,
        jnp.where(positive, toward, away),
        jnp.where(positive, beyond, 0.0),
    )


def body(
    sizes, vort_hbm, vel_hbm, out, vort, vel, wgt, slope, cur, sx, rx, sy, ry, sz, rz, rvx, svy, rvy, svz, rvz,
    send_sem, recv_sem, load_sem,
):
    _, X, Y, Z = vort.shape
    here = [lax.axis_index(a) for a in AXES]

    def neighbour(k, side):
        n = sizes[k]
        moved = lax.rem(here[k] + (1 if side else n - 1), n)
        return tuple(moved if j == k else here[j] for j in range(3))

    def push(src, dst, index, k, side):
        copy = pltpu.make_async_remote_copy(
            src_ref=src, dst_ref=dst, send_sem=send_sem.at[index], recv_sem=recv_sem.at[index],
            device_id=neighbour(k, side), device_id_type=MESH,
        )
        copy.start()
        return copy

    barrier = pltpu.get_barrier_semaphore()
    for k in range(3):
        for side in range(2):
            pl.semaphore_signal(barrier, inc=1, device_id=neighbour(k, side), device_id_type=MESH)

    loads = [
        pltpu.make_async_copy(vel_hbm, vel, load_sem.at[0]),
        pltpu.make_async_copy(vort_hbm, vort, load_sem.at[1]),
    ]
    for cp in loads:
        cp.start()

    lane = lax.broadcasted_iota(jnp.int32, (8, Z), 1)
    lane3 = lax.broadcasted_iota(jnp.int32, (X, Y, Z), 2)
    row3 = lax.broadcasted_iota(jnp.int32, (X, Y, Z), 1)
    slabs = [(c, x, y) for c in range(3) for x in range(X) for y in range(0, Y, 8)]
    per = Z // 4

    def pack(edges, target):
        for m in range(0, len(slabs), per):
            held = jnp.zeros((8, Z), jnp.float32)
            for k, (c, x, y) in enumerate(slabs[m:m + per]):
                moved = roll(edges[c][x, y:y + 8, :], 4 * k + 2, 1)
                held = jnp.where(lane // 4 == k, moved, held)
            target[m // per] = held

    def unpack(low_side, high_side):
        merged = [
            jnp.where(lane % 4 >= 2, low_side[m], high_side[m])
            for m in range(-(-len(slabs) // per))
        ]
        edge = (lane < 2) | (lane >= Z - 2)
        return [
            jnp.where(edge, roll(merged[i // per], -(4 * (i % per) + 2), 1), 0.0)
            for i in range(len(slabs))
        ]

    def spread_x(src, step):
        for c in range(3):
            w = [wgt.at[0, a] for a in range(5)]
            sx[step, 0, c, 0] = w[0][0] * src[c, 0]
            sx[step, 0, c, 1] = w[1][0] * src[c, 0] + w[0][1] * src[c, 1]
            sx[step, 1, c, 0] = w[3][X - 1] * src[c, X - 1] + w[4][X - 2] * src[c, X - 2]
            sx[step, 1, c, 1] = w[4][X - 1] * src[c, X - 1]

    def interior_x(src):
        for c in range(3):
            layers = []
            for x in range(X):
                total = None
                for a in range(-2, 3):
                    if 0 <= x - a < X:
                        term = wgt[0, a + 2, x - a] * src[c, x - a]
                        total = term if total is None else total + term
                layers.append(total)
            for x in range(X):
                yield c, x, layers[x]

    def put_weights(k):
        for a, w in enumerate(weights(vel[k])):
            wgt[k, a] = w

    loads[0].wait()
    put_weights(0)
    loads[1].wait()
    spread_x(vort, 0)
    pl.semaphore_wait(barrier, 6)
    pending = []
    first = [push(sx.at[0, s], rx.at[0, s], s, 0, s) for s in range(2)]
    for s in range(2):
        svy[s] = vel[:, :, pl.ds((Y - 2) * s, 2), :]
    pack([vel[c] for c in range(3)], svz)
    vy = [push(svy.at[s], rvy.at[s], 14 + s, 1, s) for s in range(2)]
    vz = [push(svz, rvz.at[s], 16 + s, 2, s) for s in range(2)]
    vx = [push(vel.at[:, pl.ds((X - 2) * s, 2)], rvx.at[s], 12 + s, 0, s) for s in range(2)]
    put_weights(1)
    put_weights(2)

    scale = TIME_STEP / 12.0

    def slopes_y():
        for c in range(3):
            v = vel[c]
            near = 8.0 * (roll(v, -1, 1) - roll(v, 1, 1)) - (roll(v, -2, 1) - roll(v, 2, 1))
            slope[1, c] = near * scale
        for cp in vy:
            cp.wait()
        for c in range(3):
            top = vel[c, :, 0:4, :]
            low = rvy[1, c]
            slope[1, c, :, 0:1, :] = scale * (
                8.0 * (top[:, 1:2] - low[:, 1:2]) - (top[:, 2:3] - low[:, 0:1]))
            slope[1, c, :, 1:2, :] = scale * (
                8.0 * (top[:, 2:3] - top[:, 0:1]) - (top[:, 3:4] - low[:, 1:2]))
            end = vel[c, :, Y - 4:Y, :]
            high = rvy[0, c]
            slope[1, c, :, Y - 2:Y - 1, :] = scale * (
                8.0 * (end[:, 3:4] - end[:, 1:2]) - (high[:, 0:1] - end[:, 0:1]))
            slope[1, c, :, Y - 1:Y, :] = scale * (
                8.0 * (high[:, 0:1] - end[:, 2:3]) - (high[:, 1:2] - end[:, 1:2]))

    def slopes_z():
        for cp in vz:
            cp.wait()
        halo = unpack(rvz.at[0], rvz.at[1])
        for i, (c, x, y) in enumerate(slabs):
            v = vel[c, x, y:y + 8, :]
            h = halo[i]

            def at(shift):
                source = roll(v, -shift, 1)
                if shift > 0:
                    return jnp.where(lane >= Z - shift, roll(h, -shift, 1), source)
                return jnp.where(lane < -shift, roll(h, -shift, 1), source)

            slope[2, c, x, y:y + 8, :] = scale * (8.0 * (at(1) - at(-1)) - (at(2) - at(-2)))

    def slopes_x():
        for cp in vx:
            cp.wait()
        for c in range(3):
            def layer(x):
                if x < 0:
                    return rvx[1, c, x + 2]
                if x >= X:
                    return rvx[0, c, x - X]
                return vel[c, x]
            for x in range(X):
                slope[0, c, x] = scale * (
                    8.0 * (layer(x + 1) - layer(x - 1)) - (layer(x + 2) - layer(x - 2)))

    for step in range(SUBSTEPS):
        base = step * 6
        src = vort if step == 0 else cur
        if step > 0:
            spread_x(src, step)
            first = [push(sx.at[step, s], rx.at[step, s], base + s, 0, s) for s in range(2)]
        for c, x, layer in interior_x(src):
            cur[c, x] = layer
        if step == 0:
            slopes_y()
            slopes_z()
        for cp in first:
            cp.wait()
        for c in range(3):
            for x in range(2):
                cur[c, x] += rx[step, 1, c, x]
                cur[c, X - 2 + x] += rx[step, 0, c, x]

        for c in range(3):
            v = cur[c]
            u = [wgt[1, a] * v for a in range(5)]
            keep, go = u[2], None
            for a in (-2, -1, 1, 2):
                moved = roll(u[a + 2], a, 1)
                outside = row3 < a if a > 0 else row3 >= Y + a
                keep = keep + jnp.where(outside, 0.0, moved)
                part = jnp.where(outside, moved, 0.0)
                go = part if go is None else go + part
            cur[c] = keep
            sy[step, 1, c] = go[:, 0:2, :]
            sy[step, 0, c] = go[:, Y - 2:Y, :]
        copies = [push(sy.at[step, s], ry.at[step, s], base + 2 + s, 1, s) for s in range(2)]
        if step == 0:
            slopes_x()
        for cp in copies:
            cp.wait()
        for c in range(3):
            cur[c, :, 0:2, :] += ry[step, 1, c]
            cur[c, :, Y - 2:Y, :] += ry[step, 0, c]

        edges = []
        for c in range(3):
            v = cur[c]
            u = [wgt[2, a] * v for a in range(5)]
            keep, go = u[2], None
            for a in (-2, -1, 1, 2):
                moved = roll(u[a + 2], a, 2)
                outside = lane3 < a if a > 0 else lane3 >= Z + a
                keep = keep + jnp.where(outside, 0.0, moved)
                part = jnp.where(outside, moved, 0.0)
                go = part if go is None else go + part
            cur[c] = keep
            edges.append(go)
        pack(edges, sz.at[step])
        copies = [push(sz.at[step], rz.at[step, s], base + 4 + s, 2, s) for s in range(2)]
        for cp in copies:
            cp.wait()
        halo = unpack(rz.at[step, 1], rz.at[step, 0])
        final = out if step == SUBSTEPS - 1 else cur
        for x in range(X):
            for y in range(0, Y, 8):
                v = [
                    cur[c, x, y:y + 8, :] + halo[slabs.index((c, x, y))]
                    for c in range(3)
                ]
                for i in range(3):
                    total = v[i]
                    for j in range(3):
                        total = total + v[j] * slope[j, i, x, y:y + 8, :]
                    final[i, x, y:y + 8, :] = total


def solution(mesh):
    sizes = [mesh.shape[a] for a in AXES]

    def local(vort, vel):
        _, X, Y, Z = vort.shape
        packs = -(-(3 * X * (Y // 8)) // (Z // 4))
        f32 = jnp.float32
        V = pltpu.VMEM
        S = SUBSTEPS
        return pl.pallas_call(
            functools.partial(body, sizes),
            out_shape=V(vort.shape, f32),
            in_specs=[pl.BlockSpec(memory_space=pl.ANY)] * 2,
            out_specs=pl.BlockSpec(memory_space=pltpu.VMEM),
            scratch_shapes=[
                V(vort.shape, f32),
                V(vort.shape, f32),
                V((3, 5, X, Y, Z), f32),
                V((3, 3, X, Y, Z), f32),
                V((3, X, Y, Z), f32),
                V((S, 2, 3, 2, Y, Z), f32),
                V((S, 2, 3, 2, Y, Z), f32),
                V((S, 2, 3, X, 2, Z), f32),
                V((S, 2, 3, X, 2, Z), f32),
                V((S, packs, 8, Z), f32),
                V((S, 2, packs, 8, Z), f32),
                V((2, 3, 2, Y, Z), f32),
                V((2, 3, X, 2, Z), f32),
                V((2, 3, X, 2, Z), f32),
                V((packs, 8, Z), f32),
                V((2, packs, 8, Z), f32),
                pltpu.SemaphoreType.DMA((18,)),
                pltpu.SemaphoreType.DMA((18,)),
                pltpu.SemaphoreType.DMA((2,)),
            ],
            compiler_params=pltpu.CompilerParams(collective_id=0, has_side_effects=True),
        )(vort, vel)

    placed = P(None, *AXES)
    return jax.shard_map(
        local, mesh=mesh, in_specs=(placed, placed), out_specs=placed, check_vma=False
    )
```

```python
import functools

import jax
import jax.numpy as jnp
from jax import lax
from jax.experimental import pallas as pl
from jax.experimental.pallas import tpu as pltpu
from jax.sharding import PartitionSpec as P

SUBSTEPS = 2
TIME_STEP = 0.5
AXES = ("gx", "gy", "gz")
MESH = pl.DeviceIdType.MESH
SIDES = (-1, 1)


def roll(values, shift, axis):
    shift %= values.shape[axis]
    return pltpu.roll(values, shift, axis) if shift else values


def weights(velocity):
    d = TIME_STEP * velocity
    s = jnp.abs(d)
    t = 1.0 - s
    positive = d > 0.0
    centre = 1.0 + s * s * (1.5 * s - 2.5)
    toward = 1.0 + t * t * (1.5 * t - 2.5)
    away = -0.5 * s * t * t
    beyond = -0.5 * s * s * t
    return (
        jnp.where(positive, 0.0, beyond),
        jnp.where(positive, away, toward),
        centre,
        jnp.where(positive, toward, away),
        jnp.where(positive, beyond, 0.0),
    )


def inside(w, a, index, extent):
    if a == 0:
        return w
    return jnp.where(index < extent - a if a > 0 else index >= -a, w, 0.0)


def body(
    sizes, vort_hbm, vel_hbm, out, vort, vel, wgt, wgt_y, slope, cur,
    qvort, qvel, qcur, qwgt, qwgt_y, qslope,
    sx, rx, sy, ry, sxy, rxy, rvx, svy, rvy, sz, rz,
    sxq, rxq, syq, ryq, sxyq, rxyq,
    send_sem, recv_sem, load_sem,
):
    _, X, Y, Z = vort.shape
    W = Z // X
    assert W * X == Z and W >= 16 and X >= 6 and Y >= 8
    scale = TIME_STEP / 12.0
    here = [lax.axis_index(a) for a in AXES]

    def device(*offset):
        return tuple(
            here[k] if not d else lax.rem(here[k] + (d % sizes[k]), sizes[k])
            for k, d in enumerate(offset)
        )

    pushed = []

    def push(src, dst, offset):
        index = len(pushed)
        copy = pltpu.make_async_remote_copy(
            src_ref=src, dst_ref=dst, send_sem=send_sem.at[index], recv_sem=recv_sem.at[index],
            device_id=device(*offset), device_id_type=MESH,
        )
        copy.start()
        pushed.append(copy)
        return copy

    def arrived(copies):
        for copy in copies:
            copy.wait_recv()

    plane = [(dx, dy, 0) for dx in (-1, 0, 1) for dy in (-1, 0, 1) if dx or dy]
    greeted = plane + [(0, 0, -1)]
    barrier = pltpu.get_barrier_semaphore()
    for offset in greeted:
        pl.semaphore_signal(barrier, inc=1, device_id=device(*offset), device_id_type=MESH)
    loads = [
        pltpu.make_async_copy(vel_hbm, vel, load_sem.at[0]),
        pltpu.make_async_copy(vort_hbm, vort, load_sem.at[1]),
    ]
    for cp in loads:
        cp.start()

    lane = lax.broadcasted_iota(jnp.int32, (Y, Z), 1)
    row = lax.broadcasted_iota(jnp.int32, (Y, Z), 0)
    cell = lane % W
    edge = (lane < 2) | (lane >= Z - 2)

    def strip(src, c):
        held = roll(src[c, 0], 4, 1)
        for x in range(1, X):
            held = jnp.where(lane >= W * x, roll(src[c, x], W * x + 4, 1), held)
        return held

    def spread_x(src, step):
        w = [wgt.at[0, a] for a in range(5)]
        for c in range(3):
            sx[step, 0, c, 0] = w[0][0] * src[c, 0]
            sx[step, 0, c, 1] = w[1][0] * src[c, 0] + w[0][1] * src[c, 1]
            sx[step, 1, c, 0] = w[3][X - 1] * src[c, X - 1] + w[4][X - 2] * src[c, X - 2]
            sx[step, 1, c, 1] = w[4][X - 1] * src[c, X - 1]
            for s in range(2):
                for t in range(2):
                    sxy[step, s, t, c] = sx[step, s, c, :, pl.ds((Y - 2) * t, 2), :]

    def push_x(step):
        copies = [push(sx.at[step, s], rx.at[step, s], (SIDES[s], 0, 0)) for s in range(2)]
        copies += [
            push(sxy.at[step, s, t], rxy.at[step, s, t], (SIDES[s], SIDES[t], 0))
            for s in range(2) for t in range(2)
        ]
        return copies

    def interior_x(src, step):
        for c in range(3):
            layers = []
            for x in range(X):
                total = None
                for a in range(-2, 3):
                    if 0 <= x - a < X:
                        term = wgt[0, a + 2, x - a] * src[c, x - a]
                        total = term if total is None else total + term
                layers.append(total)
            for x in range(X):
                cur[c, x] = layers[x]
                for t in range(2):
                    sy[step, t, c, x] = layers[x][(Y - 2) * t:(Y - 2) * t + 2]

    def push_y(step):
        return [push(sy.at[step, t], ry.at[step, t], (0, SIDES[t], 0)) for t in range(2)]

    def put_weights(k):
        for x in range(X):
            for a, w in enumerate(weights(vel[k, x])):
                if k == 1:
                    w = inside(w, a - 2, row, Y)
                if k == 2:
                    w = inside(w, a - 2, lane, Z)
                wgt[k, a, x] = w

    def chunks(values, side):
        held = None
        for c in range(3):
            moved = roll(values[c], 2 * W * (c if side else c + 1), 1)
            held = moved if held is None else jnp.where(lane >= 2 * W * c, moved, held)
        return held

    def unchunk(first, last, c):
        n = first.shape[0]
        low = roll(first, -2 * W * c, 1)
        high = roll(last, Z - 2 * W - 2 * W * c, 1)
        at = lane[:n]
        return jnp.where(at < 2 * W, low, jnp.where(at >= Z - 2 * W, high, 0.0))

    def strip_x(src, step):
        went = []
        for c in range(3):
            u = [qwgt[0, a] * src[c] for a in range(5)]
            keep, go = u[2], None
            for a in (-2, -1, 1, 2):
                moved = roll(u[a + 2], W * a, 1)
                outside = lane < W * a if a > 0 else lane >= W * (X + a)
                keep = keep + jnp.where(outside, 0.0, moved)
                part = jnp.where(outside, moved, 0.0)
                go = part if go is None else go + part
            qcur[c] = keep
            went.append(go)
            for t in range(2):
                syq[step, t, c] = keep[(Y - 2) * t:(Y - 2) * t + 2]
        for s in range(2):
            held = chunks(went, s)
            sxq[step, s, 0] = held
            for t in range(2):
                sxyq[step, s, t] = held[(Y - 2) * t:(Y - 2) * t + 2]

    def push_strip(step):
        n = 2 if step == 0 else 1
        copies = [
            push(sxq.at[step, s, pl.ds(0, n)], rxq.at[step, s, pl.ds(0, n)], (SIDES[s], 0, 0))
            for s in range(2)
        ]
        copies += [
            push(syq.at[step, t, pl.ds(0, 3 * n)], ryq.at[step, t, pl.ds(0, 3 * n)], (0, SIDES[t], 0))
            for t in range(2)
        ]
        copies += [
            push(sxyq.at[step, s, t], rxyq.at[step, s, t], (SIDES[s], SIDES[t], 0))
            for s in range(2) for t in range(2)
        ]
        return copies

    def pass_y(step):
        for c in range(3):
            for x in range(2):
                cur[c, x] += rx[step, 1, c, x]
                cur[c, X - 2 + x] += rx[step, 0, c, x]
        for c in range(3):
            for x in range(X):
                v = cur[c, x]
                total = wgt[1, 2, x] * v
                for a in (-2, -1, 1, 2):
                    total = total + roll(wgt[1, a + 2, x] * v, a, 0)
                low, high = ry[step, 1, c, x], ry[step, 0, c, x]
                if x < 2:
                    low = low + rxy[step, 1, 1, c, x]
                    high = high + rxy[step, 1, 0, c, x]
                if x >= X - 2:
                    low = low + rxy[step, 0, 1, c, x - X + 2]
                    high = high + rxy[step, 0, 0, c, x - X + 2]
                total = pass_z(x, total, low, high)
                cur[c, x] = total

    def ends(total, low, high, w):
        near = w[0] * low
        first = w[1] * low + jnp.concatenate([near[1:2], jnp.zeros_like(near[:1])], 0)
        near = w[2] * high
        last = w[3] * high + jnp.concatenate([jnp.zeros_like(near[:1]), near[0:1]], 0)
        gap = jnp.zeros((Y - 4, Z), jnp.float32)
        return total + jnp.concatenate([first, gap, last], 0)

    def pass_z(x, v, low, high):
        v = ends(v, low, high, [wgt_y[i, x] for i in range(4)])
        total = wgt[2, 2, x] * v
        for a in (-2, -1, 1, 2):
            total = total + roll(wgt[2, a + 2, x] * v, a, 1)
        return total

    def strip_yz(step):
        reach = []
        for c in range(3):
            v = qcur[c] + unchunk(rxq[step, 1, 0], rxq[step, 0, 0], c)
            total = qwgt[1, 2] * v
            for a in (-2, -1, 1, 2):
                total = total + roll(qwgt[1, a + 2] * v, a, 0)
            low = ryq[step, 1, c] + corner(step, 1, c)
            high = ryq[step, 0, c] + corner(step, 0, c)
            v = ends(total, low, high, [qwgt_y[i] for i in range(4)])
            moved = [roll(qwgt[2, a + 2] * v, a, 1) for a in range(-2, 3)]
            low = jnp.where(cell == 4, moved[3], 0.0) + moved[4]
            high = jnp.where(cell == 11, moved[1], 0.0) + moved[0]
            reach.append(jnp.where(cell >= 4, low, roll(high, -8, 1)))
            if step == 0:
                qcur[c] = moved[0] + moved[1] + moved[2] + moved[3] + moved[4]
        return reach

    def corner(step, t, c):
        first = jnp.concatenate([rxyq[step, 1, t]] * 4, 0)
        last = jnp.concatenate([rxyq[step, 0, t]] * 4, 0)
        return unchunk(first, last, c)[:2]

    def slope_rows(v, axis):
        return scale * (
            8.0 * (roll(v, -1, axis) - roll(v, 1, axis)) - (roll(v, -2, axis) - roll(v, 2, axis)))

    def slope_ends(dst, v, low, high):
        top, end = v[0:4], v[Y - 4:Y]
        dst[0:1] = scale * (8.0 * (top[1:2] - low[1:2]) - (top[2:3] - low[0:1]))
        dst[1:2] = scale * (8.0 * (top[2:3] - top[0:1]) - (top[3:4] - low[1:2]))
        dst[Y - 2:Y - 1] = scale * (8.0 * (end[3:4] - end[1:2]) - (high[0:1] - end[0:1]))
        dst[Y - 1:Y] = scale * (8.0 * (high[0:1] - end[2:3]) - (high[1:2] - end[1:2]))

    def slope_x(layers):
        for c in range(3):
            def layer(x):
                if x < 0:
                    return rvx[1, c, x + 2]
                if x >= X:
                    return rvx[0, c, x - X]
                return vel[c, x]
            for x in layers:
                slope[0, c, x] = scale * (
                    8.0 * (layer(x + 1) - layer(x - 1)) - (layer(x + 2) - layer(x - 2)))

    loads[0].wait()
    put_weights(0)
    loads[1].wait()
    spread_x(vort, 0)
    strips = [strip(vort, c) for c in range(3)] + [strip(vel, c) for c in range(3)]
    for m in range(2):
        up = down = None
        for j, s in enumerate(strips[4 * m:4 * m + 4]):
            moved = roll(s, 4 * j, 1), roll(s, 4 * j - 4, 1)
            up = moved[0] if up is None else jnp.where(cell >= 4 * j, moved[0], up)
            down = moved[1] if down is None else jnp.where(cell >= 4 * j, moved[1], down)
        sz[1, m] = up
        sz[0, m] = down
    for c in range(3):
        qvort[c] = jnp.where(cell < 8, strips[c], roll(strips[c], 8, 1))
        qvel[c] = jnp.where(cell < 8, strips[3 + c], roll(strips[3 + c], 8, 1))
    for t in range(2):
        svy[t] = vel[:, :, pl.ds((Y - 2) * t, 2), :]
    pl.semaphore_wait(barrier, len(greeted))
    z_up = push(sz.at[1], rz.at[1], (0, 0, 1))
    from_x = push_x(0)
    vel_y = [push(svy.at[t], rvy.at[t], (0, SIDES[t], 0)) for t in range(2)]
    interior_x(vort, 0)
    from_y = push_y(0)
    vel_x = [
        push(vel.at[:, pl.ds((X - 2) * s, 2)], rvx.at[s], (SIDES[s], 0, 0)) for s in range(2)
    ]
    z_up.wait_recv()
    z_down = push(sz.at[0], rz.at[0], (0, 0, -1))
    put_weights(1)
    put_weights(2)
    for c in range(3):
        for x in range(X):
            slope[1, c, x] = slope_rows(vel[c, x], 0)
            slope[2, c, x] = slope_rows(vel[c, x], 1)
    slope_x(range(2, X - 2))

    z_down.wait_recv()
    for i in range(6):
        m, j = divmod(i, 4)
        low = roll(rz[1, m], -4 * j, 1)
        high = roll(rz[0, m], 12 - 4 * j, 1)
        dst = (qvort if i < 3 else qvel).at[i % 3]
        dst[...] = jnp.where(cell < 4, low, jnp.where(cell >= 12, high, dst[...]))
    for k in range(3):
        for a, w in enumerate(weights(qvel[k])):
            qwgt[k, a] = inside(w, a - 2, row, Y) if k == 1 else w
    strip_x([qvort[c] for c in range(3)], 0)
    for s in range(2):
        sxq[0, s, 1] = chunks([qvel[c] for c in range(3)], 1 - s)
    for t in range(2):
        syq[0, t, pl.ds(3, 3)] = qvel[:, pl.ds((Y - 2) * t, 2), :]
    from_strip = push_strip(0)
    for c in range(3):
        v = qvel[c]
        qslope[1, c] = slope_rows(v, 0)
        qslope[2, c] = slope_rows(v, 1)

    arrived(vel_y)
    for x in range(X):
        low, high = weights(rvy[1, 1, x]), weights(rvy[0, 1, x])
        for i, w in enumerate((low[3], low[4], high[1], high[0])):
            wgt_y[i, x] = w
    for c in range(3):
        for x in range(X):
            slope_ends(slope.at[1, c, x], vel[c, x], rvy[1, c, x], rvy[0, c, x])

    for step in range(SUBSTEPS):
        last = step == SUBSTEPS - 1
        arrived(from_y)
        arrived(from_x)
        pass_y(step)
        if step == 0:
            arrived(vel_x)
            slope_x([0, 1, X - 2, X - 1])
        arrived(from_strip)
        if step == 0:
            low, high = weights(ryq[0, 1, 4]), weights(ryq[0, 0, 4])
            for i, w in enumerate((low[3], low[4], high[1], high[0])):
                qwgt_y[i] = w
        reach = strip_yz(step)
        if step == 0:
            steep = []
            for c in range(3):
                v = qvel[c]
                h = unchunk(rxq[0, 0, 1], rxq[0, 1, 1], c)

                def at(shift):
                    source = roll(v, -W * shift, 1)
                    beyond = lane >= Z - W * shift if shift > 0 else lane < -W * shift
                    return jnp.where(beyond, roll(h, -W * shift, 1), source)

                qslope[0, c] = scale * (8.0 * (at(1) - at(-1)) - (at(2) - at(-2)))
                slope_ends(qslope.at[1, c], v, ryq[0, 1, 3 + c], ryq[0, 0, 3 + c])
                steep.append(jnp.where(cell >= 4, qslope[2, c], roll(qslope[2, c], -8, 1)))
            v = [qcur[c] for c in range(3)]
            for i in range(3):
                total = v[i]
                for j in range(3):
                    total = total + v[j] * qslope[j, i]
                qcur[i] = total

        final = out if last else cur
        order = [0, 1, X - 2, X - 1] + list(range(2, X - 2))
        for n, x in enumerate(order):
            if n == 4 and not last:
                spread_x(cur, step + 1)
                from_x = push_x(step + 1)
            v = [
                cur[c, x] + jnp.where(edge, roll(reach[c], -(W * x + 4), 1), 0.0)
                for c in range(3)
            ]
            if step == 0:
                for c in range(3):
                    slope[2, c, x] = jnp.where(
                        edge, roll(steep[c], -(W * x + 4), 1), slope[2, c, x])
            for i in range(3):
                total = v[i]
                for j in range(3):
                    total = total + v[j] * slope[j, i, x]
                final[i, x] = total
        if not last:
            strip_x([qcur[c] for c in range(3)], step + 1)
            from_strip = push_strip(step + 1)
            interior_x(cur, step + 1)
            from_y = push_y(step + 1)
    for copy in pushed:
        copy.wait_send()


def solution(mesh):
    sizes = [mesh.shape[a] for a in AXES]

    def local(vort, vel):
        _, X, Y, Z = vort.shape
        S = SUBSTEPS

        def V(*shape):
            return pltpu.VMEM(shape, jnp.float32)

        return pl.pallas_call(
            functools.partial(body, sizes),
            out_shape=V(*vort.shape),
            in_specs=[pl.BlockSpec(memory_space=pl.ANY)] * 2,
            out_specs=pl.BlockSpec(memory_space=pltpu.VMEM),
            scratch_shapes=[
                V(3, X, Y, Z), V(3, X, Y, Z),
                V(3, 5, X, Y, Z), V(4, X, 2, Z), V(3, 3, X, Y, Z), V(3, X, Y, Z),
                V(3, Y, Z), V(3, Y, Z), V(3, Y, Z), V(3, 5, Y, Z), V(4, 2, Z), V(3, 3, Y, Z),
                V(S, 2, 3, 2, Y, Z), V(S, 2, 3, 2, Y, Z),
                V(S, 2, 3, X, 2, Z), V(S, 2, 3, X, 2, Z),
                V(S, 2, 2, 3, 2, 2, Z), V(S, 2, 2, 3, 2, 2, Z),
                V(2, 3, 2, Y, Z),
                V(2, 3, X, 2, Z), V(2, 3, X, 2, Z),
                V(2, 2, Y, Z), V(2, 2, Y, Z),
                V(S, 2, 2, Y, Z), V(S, 2, 2, Y, Z),
                V(S, 2, 6, 2, Z), V(S, 2, 6, 2, Z),
                V(S, 2, 2, 2, Z), V(S, 2, 2, 2, Z),
                pltpu.SemaphoreType.DMA((40,)),
                pltpu.SemaphoreType.DMA((40,)),
                pltpu.SemaphoreType.DMA((2,)),
            ],
            compiler_params=pltpu.CompilerParams(collective_id=0, has_side_effects=True),
        )(vort, vel)

    placed = P(None, *AXES)
    return jax.shard_map(
        local, mesh=mesh, in_specs=(placed, placed), out_specs=placed, check_vma=False
    )
```

```python
import functools

import jax
import jax.numpy as jnp
from jax import lax
from jax.experimental import pallas as pl
from jax.experimental.pallas import tpu as pltpu
from jax.sharding import PartitionSpec as P

SUBSTEPS = 2
TIME_STEP = 0.5
AXES = ("gx", "gy", "gz")
MESH = pl.DeviceIdType.MESH
SIDES = (-1, 1)


def roll(values, shift, axis):
    shift %= values.shape[axis]
    return pltpu.roll(values, shift, axis) if shift else values


def weights(velocity):
    d = TIME_STEP * velocity
    s = jnp.abs(d)
    t = 1.0 - s
    positive = d > 0.0
    centre = 1.0 + s * s * (1.5 * s - 2.5)
    toward = 1.0 + t * t * (1.5 * t - 2.5)
    away = -0.5 * s * t * t
    beyond = -0.5 * s * s * t
    return (
        jnp.where(positive, 0.0, beyond),
        jnp.where(positive, away, toward),
        centre,
        jnp.where(positive, toward, away),
        jnp.where(positive, beyond, 0.0),
    )


def inside(w, a, index, extent):
    if a == 0:
        return w
    return jnp.where(index < extent - a if a > 0 else index >= -a, w, 0.0)


def body(
    sizes, vort_hbm, vel_hbm, out, vort, vel, wgt, wgt_y, slope, cur,
    strip, ext, wgt_s, slope_s,
    sx, rx, sy, ry, sxy, rxy, rvx, svy, rvy, sz, rz, ssx, rsx, ssy, rsy, ssxy, rsxy,
    send_sem, recv_sem, load_sem,
):
    _, X, Y, Z = vort.shape
    W = 8
    H = 4 * W
    assert (X + 8) * W == Z and 2 * H + X * W == Z and Y >= 8
    scale = TIME_STEP / 12.0
    here = [lax.axis_index(a) for a in AXES]

    def device(*offset):
        return tuple(
            here[k] if not d else lax.rem(here[k] + (d % sizes[k]), sizes[k])
            for k, d in enumerate(offset)
        )

    pushed = []

    def push(src, dst, offset, start=True):
        index = len(pushed)
        copy = pltpu.make_async_remote_copy(
            src_ref=src, dst_ref=dst, send_sem=send_sem.at[index], recv_sem=recv_sem.at[index],
            device_id=device(*offset), device_id_type=MESH,
        )
        if start:
            copy.start()
        pushed.append(copy)
        return copy

    def arrived(copies):
        for copy in copies:
            copy.wait_recv()

    plane = [(dx, dy, 0) for dx in (-1, 0, 1) for dy in (-1, 0, 1) if dx or dy]
    bottom, top = here[2] == 0, here[2] == sizes[2] - 1
    barrier = pltpu.get_barrier_semaphore()

    def greet(offset):
        pl.semaphore_signal(barrier, inc=1, device_id=device(*offset), device_id_type=MESH)

    for offset in plane:
        greet(offset)
    greet((0, 0, -1))

    @pl.when(jnp.logical_not(top))
    def _():
        greet((0, 0, 1))

    loads = [
        pltpu.make_async_copy(vel_hbm, vel, load_sem.at[0]),
        pltpu.make_async_copy(vort_hbm, vort, load_sem.at[1]),
    ]
    for cp in loads:
        cp.start()

    wide = lax.broadcasted_iota(jnp.int32, (Y + 8, Z), 1)
    lane = lax.broadcasted_iota(jnp.int32, (Y, Z), 1)
    row = lax.broadcasted_iota(jnp.int32, (Y, Z), 0)
    cell = lane % W
    edge = (lane < 2) | (lane >= Z - 2)
    rim = (lane < 4) | (lane >= Z - 4)

    def faces(src, c):
        found = roll(src[c, 0], H + 4, 1)
        for x in range(1, X):
            found = jnp.where(lane >= H + W * x, roll(src[c, x], H + W * x + 4, 1), found)
        return found

    def spread_x(src, step, s):
        for c in range(3):
            if s == 0:
                sx[step, 0, c, 0] = wgt[0, 0, 0] * src[c, 0]
                sx[step, 0, c, 1] = wgt[0, 1, 0] * src[c, 0] + wgt[0, 0, 1] * src[c, 1]
            else:
                sx[step, 1, c, 0] = (
                    wgt[0, 3, X - 1] * src[c, X - 1] + wgt[0, 4, X - 2] * src[c, X - 2])
                sx[step, 1, c, 1] = wgt[0, 4, X - 1] * src[c, X - 1]
            for t in range(2):
                sxy[step, s, t, c] = sx[step, s, c, :, pl.ds((Y - 2) * t, 2), :]

    def push_x(step, s):
        return [push(sx.at[step, s], rx.at[step, s], (SIDES[s], 0, 0))] + [
            push(sxy.at[step, s, t], rxy.at[step, s, t], (SIDES[s], SIDES[t], 0))
            for t in range(2)
        ]

    def interior_x(src, step):
        for c in range(3):
            layers = []
            for x in range(X):
                total = None
                for a in range(-2, 3):
                    if 0 <= x - a < X:
                        term = wgt[0, a + 2, x - a] * src[c, x - a]
                        total = term if total is None else total + term
                layers.append(total)
            for x in range(X):
                cur[c, x] = layers[x]
                for t in range(2):
                    sy[step, t, c, x] = layers[x][(Y - 2) * t:(Y - 2) * t + 2]

    def push_y(step):
        return [push(sy.at[step, t], ry.at[step, t], (0, SIDES[t], 0)) for t in range(2)]

    def put_weights(k):
        for x in range(X):
            for a, w in enumerate(weights(vel[k, x])):
                if k == 1:
                    w = inside(w, a - 2, row, Y)
                if k == 2:
                    w = inside(w, a - 2, lane, Z)
                wgt[k, a, x] = w

    def ends(total, low, high, w):
        near = w[0] * low
        first = w[1] * low + jnp.concatenate([near[1:2], jnp.zeros_like(near[:1])], 0)
        near = w[2] * high
        last = w[3] * high + jnp.concatenate([jnp.zeros_like(near[:1]), near[0:1]], 0)
        gap = jnp.zeros((Y - 4, Z), jnp.float32)
        return total + jnp.concatenate([first, gap, last], 0)

    def pass_yz(step, x):
        after = []
        for c in range(3):
            v = cur[c, x]
            low, high = ry[step, 1, c, x], ry[step, 0, c, x]
            for s, i in ((1, x), (0, x - X + 2)):
                if 0 <= i < 2:
                    v = v + rx[step, s, c, i]
                    low = low + rxy[step, s, 1, c, i]
                    high = high + rxy[step, s, 0, c, i]
            total = wgt[1, 2, x] * v
            for a in (-2, -1, 1, 2):
                total = total + roll(wgt[1, a + 2, x] * v, a, 0)
            v = ends(total, low, high, [wgt_y[i, x] for i in range(4)])
            if step > 0:
                v = jnp.where(edge, 0.0, v)
            total = wgt[2, 2, x] * v
            for a in (-2, -1, 1, 2):
                total = total + roll(wgt[2, a + 2, x] * v, a, 1)
            after.append(total)
        return after

    def stretch(v, steepness):
        total = []
        for i in range(3):
            t = v[i]
            for j in range(3):
                t = t + v[j] * steepness(j, i)
            total.append(t)
        return total

    def passes(values, w, axes):
        for k, axis, size in axes:
            total = w(k, 2) * values
            for a in (-2, -1, 1, 2):
                total = total + roll(w(k, a + 2) * values, size * a, axis)
            values = total
        return values

    def slope_rows(v, axis, n=1):
        near = roll(v, -n, axis) - roll(v, n, axis)
        return scale * (8.0 * near - (roll(v, -2 * n, axis) - roll(v, 2 * n, axis)))

    def slope_ends(dst, v, low, high):
        top, end = v[0:4], v[Y - 4:Y]
        dst[0:1] = scale * (8.0 * (top[1:2] - low[1:2]) - (top[2:3] - low[0:1]))
        dst[1:2] = scale * (8.0 * (top[2:3] - top[0:1]) - (top[3:4] - low[1:2]))
        dst[Y - 2:Y - 1] = scale * (8.0 * (end[3:4] - end[1:2]) - (high[0:1] - end[0:1]))
        dst[Y - 1:Y] = scale * (8.0 * (high[0:1] - end[2:3]) - (high[1:2] - end[1:2]))

    def slope_x(layers):
        for c in range(3):
            def layer(x):
                if x < 0:
                    return rvx[1, c, x + 2]
                if x >= X:
                    return rvx[0, c, x - X]
                return vel[c, x]
            for x in layers:
                slope[0, c, x] = scale * (
                    8.0 * (layer(x + 1) - layer(x - 1)) - (layer(x + 2) - layer(x - 2)))

    loads[0].wait()
    put_weights(0)
    loads[1].wait()
    own = [faces(vort, c) for c in range(3)] + [faces(vel, c) for c in range(3)]
    middle = (lane >= H) & (lane < Z - H)
    for i in range(6):
        strip[i] = own[i]
    for m in range(3):
        sz[m] = jnp.where(middle, own[2 * m], roll(own[2 * m + 1], 2 * H, 1))
    for s in (1, 0):
        spread_x(vort, 0, s)
    for t in range(2):
        svy[t] = vel[:, :, pl.ds((Y - 2) * t, 2), :]
    pl.semaphore_wait(barrier, len(plane) + 1 + jnp.where(bottom, 0, 1))
    z_up = push(sz, rz.at[1], (0, 0, 1))
    z_down = push(sz, rz.at[0], (0, 0, -1), start=False)

    @pl.when(jnp.logical_not(bottom))
    def _():
        z_down.start()

    from_x = {}
    for s in (1, 0):
        from_x[s] = push_x(0, s)
        from_x[s].append(
            push(vel.at[:, pl.ds((X - 2) * s, 2)], rvx.at[s], (SIDES[s], 0, 0)))
    vel_y = [push(svy.at[t], rvy.at[t], (0, SIDES[t], 0)) for t in range(2)]
    interior_x(vort, 0)
    from_y = push_y(0)
    put_weights(1)
    put_weights(2)
    for c in range(3):
        for x in range(X):
            slope[1, c, x] = slope_rows(vel[c, x], 0)
            slope[2, c, x] = slope_rows(vel[c, x], 1)
    slope_x(range(2, X - 2))
    arrived(vel_y)
    for x in range(X):
        low, high = weights(rvy[1, 1, x]), weights(rvy[0, 1, x])
        for i, w in enumerate((low[3], low[4], high[1], high[0])):
            wgt_y[i, x] = w
    for c in range(3):
        for x in range(X):
            slope_ends(slope.at[1, c, x], vel[c, x], rvy[1, c, x], rvy[0, c, x])

    z_up.wait_recv()

    @pl.when(bottom)
    def _():
        z_down.start()

    z_down.wait_recv()
    sides = [[], []]
    for i in range(6):
        below, above = [roll(rz[s, i // 2], 2 * H * (i % 2), 1) for s in (1, 0)]
        sides[0].append(jnp.where(cell < 4, below, strip[i]))
        sides[1].append(jnp.where(cell < 4, strip[i], above))
    both = sides[0] + sides[1]
    for i, v in enumerate(both):
        for t in range(2):
            ssy[t, i] = v[(Y - 4) * t:(Y - 4) * t + 4]
        ext[i, pl.ds(4, Y)] = v
    for s in range(2):
        for m in range(3):
            found = None
            for j in range(4):
                moved = roll(both[4 * m + j], H * (j - 1 - s), 1)
                found = moved if found is None else jnp.where(lane >= H * j, moved, found)
            ssx[s, m] = found
            for t in range(2):
                ssxy[s, t, m] = found[(Y - 4) * t:(Y - 4) * t + 4]
    from_strip = [push(ssx.at[s], rsx.at[s], (SIDES[s], 0, 0)) for s in (1, 0)]
    from_strip += [push(ssy.at[t], rsy.at[t], (0, SIDES[t], 0)) for t in range(2)]
    from_strip += [
        push(ssxy.at[s, t], rsxy.at[s, t], (SIDES[s], SIDES[t], 0))
        for s in range(2) for t in range(2)
    ]

    def advance(layers):
        for x in layers:
            v = stretch(pass_yz(0, x), lambda j, i: slope[j, i, x])
            for c in range(3):
                cur[c, x] = v[c]

    arrived(from_y)
    advance(range(2, X - 2))
    onward = {}
    for s, layers in ((1, [0, 1]), (0, [X - 2, X - 1])):
        arrived(from_x[s])
        slope_x(layers)
        advance(layers)
        spread_x(cur, 1, 1 - s)
        onward[1 - s] = push_x(1, 1 - s)
    interior_x(cur, 1)
    from_y = push_y(1)

    arrived(from_strip)
    tip = lane[:8]
    for i in range(12):
        m, j = divmod(i, 4)
        below, above = roll(rsx[1, m], -H * j, 1), roll(rsx[0, m], -H * (j + 1), 1)
        v = ext[i, pl.ds(4, Y)]
        ext[i, pl.ds(4, Y)] = jnp.where(lane < H, below, jnp.where(lane >= Z - H, above, v))
        below, above = [
            roll(jnp.concatenate([rsxy[s, 1, m], rsxy[s, 0, m]], 0), -H * (j + 1 - s), 1)
            for s in (1, 0)
        ]
        v = jnp.concatenate([rsy[1, i], rsy[0, i]], 0)
        v = jnp.where(tip < H, below, jnp.where(tip >= Z - H, above, v))
        ext[i, pl.ds(0, 4)] = v[0:4]
        ext[i, pl.ds(Y + 4, 4)] = v[4:8]
    reach = []
    held = (wide % W >= 2) & (wide % W < 6)
    for side in range(2):
        for k in range(3):
            for a, w in enumerate(weights(ext[6 * side + 3 + k])):
                wgt_s[side, k, a] = w
        for c in range(3):
            v = ext[6 * side + 3 + c]
            for k, (axis, n) in enumerate(((1, W), (0, 1), (1, 1))):
                slope_s[side, k, c] = slope_rows(v, axis, n)

        def w(k, a):
            return wgt_s[side, k, a]

        v = [
            passes(ext[6 * side + c], w, ((0, 1, W), (1, 0, 1), (2, 1, 1))) for c in range(3)
        ]
        v = stretch(v, lambda j, i: slope_s[side, j, i])
        v = [passes(u, w, ((0, 1, W), (1, 0, 1))) for u in v]
        reach.append([passes(jnp.where(held, u, 0.0), w, ((2, 1, 1),))[4:Y + 4] for u in v])
    for c in range(3):
        reach[0][c] = jnp.where(cell >= 4, reach[0][c], reach[1][c])
        steep = jnp.where(
            cell >= 4, slope_s[0, 2, c, pl.ds(4, Y)], slope_s[1, 2, c, pl.ds(4, Y)])
        for x in range(X):
            slope[2, c, x] = jnp.where(edge, roll(steep, -(H + W * x + 4), 1), slope[2, c, x])
    reach = reach[0]

    def settle(layers):
        for x in layers:
            v = pass_yz(1, x)
            for c in range(3):
                cur[c, x] = v[c]

    arrived(from_y)
    settle(range(2, X - 2))
    for s, layers in ((0, [X - 2, X - 1]), (1, [0, 1])):
        arrived(onward[s])
        settle(layers)
    for x in range(X):
        v = [
            cur[c, x] + jnp.where(rim, roll(reach[c], -(H + W * x + 4), 1), 0.0) for c in range(3)
        ]
        v = stretch(v, lambda j, i: slope[j, i, x])
        for c in range(3):
            out[c, x] = v[c]
    for copy in pushed:
        copy.wait_send()


def solution(mesh):
    sizes = [mesh.shape[a] for a in AXES]

    def local(vort, vel):
        _, X, Y, Z = vort.shape
        S = SUBSTEPS

        def V(*shape):
            return pltpu.VMEM(shape, jnp.float32)

        return pl.pallas_call(
            functools.partial(body, sizes),
            out_shape=V(*vort.shape),
            in_specs=[pl.BlockSpec(memory_space=pl.ANY)] * 2,
            out_specs=pl.BlockSpec(memory_space=pltpu.VMEM),
            scratch_shapes=[
                V(3, X, Y, Z), V(3, X, Y, Z),
                V(3, 5, X, Y, Z), V(4, X, 2, Z), V(3, 3, X, Y, Z), V(3, X, Y, Z),
                V(6, Y, Z), V(12, Y + 8, Z), V(2, 3, 5, Y + 8, Z), V(2, 3, 3, Y + 8, Z),
                V(S, 2, 3, 2, Y, Z), V(S, 2, 3, 2, Y, Z),
                V(S, 2, 3, X, 2, Z), V(S, 2, 3, X, 2, Z),
                V(S, 2, 2, 3, 2, 2, Z), V(S, 2, 2, 3, 2, 2, Z),
                V(2, 3, 2, Y, Z),
                V(2, 3, X, 2, Z), V(2, 3, X, 2, Z),
                V(3, Y, Z), V(2, 3, Y, Z),
                V(2, 3, Y, Z), V(2, 3, Y, Z),
                V(2, 12, 4, Z), V(2, 12, 4, Z),
                V(2, 2, 3, 4, Z), V(2, 2, 3, 4, Z),
                pltpu.SemaphoreType.DMA((40,)),
                pltpu.SemaphoreType.DMA((40,)),
                pltpu.SemaphoreType.DMA((2,)),
            ],
            compiler_params=pltpu.CompilerParams(collective_id=0, has_side_effects=True),
        )(vort, vel)

    placed = P(None, *AXES)
    return jax.shard_map(
        local, mesh=mesh, in_specs=(placed, placed), out_specs=placed, check_vma=False
    )
```

```python
import functools

import jax
import jax.numpy as jnp
from jax import lax
from jax.experimental import pallas as pl
from jax.experimental.pallas import tpu as pltpu
from jax.sharding import PartitionSpec as P

SUBSTEPS = 2
TIME_STEP = 0.5
AXES = ("gx", "gy", "gz")
MESH = pl.DeviceIdType.MESH
SIDES = (-1, 1)
COPIES = 46


def roll(values, shift, axis):
    shift %= values.shape[axis]
    return pltpu.roll(values, shift, axis) if shift else values


def weights(velocity):
    d = TIME_STEP * velocity
    s = jnp.abs(d)
    t = 1.0 - s
    positive = d > 0.0
    centre = 1.0 + s * s * (1.5 * s - 2.5)
    toward = 1.0 + t * t * (1.5 * t - 2.5)
    away = -0.5 * s * t * t
    beyond = -0.5 * s * s * t
    return (
        jnp.where(positive, 0.0, beyond),
        jnp.where(positive, away, toward),
        centre,
        jnp.where(positive, toward, away),
        jnp.where(positive, beyond, 0.0),
    )


def inside(w, a, index, extent):
    if a == 0:
        return w
    return jnp.where(index < extent - a if a > 0 else index >= -a, w, 0.0)


def body(
    sizes, vort_hbm, vel_hbm, out, vort, vel, wgt, wgt_y, slope, cur,
    ext, pair, wgt_s, slope_s,
    sx, rx, sy, ry, sxy, rxy, rvx, svy, rvy, sz, rz, ssx, rsx, ssy, rsy, ssxy, rsxy,
    send_sem, recv_sem, load_sem, ready,
):
    _, X, Y, Z = vort.shape
    W = 8
    H = 4 * W
    assert (X + 8) * W == Z and 2 * H + X * W == Z and Y >= 8
    scale = TIME_STEP / 12.0
    here = [lax.axis_index(a) for a in AXES]

    def device(*offset):
        return tuple(
            here[k] if not d else lax.rem(here[k] + (d % sizes[k]), sizes[k])
            for k, d in enumerate(offset)
        )

    pushed = []

    def push(src, dst, offset, start=True):
        index = len(pushed)
        copy = pltpu.make_async_remote_copy(
            src_ref=src, dst_ref=dst, send_sem=send_sem.at[index], recv_sem=recv_sem.at[index],
            device_id=device(*offset), device_id_type=MESH,
        )
        if start:
            copy.start()
        pushed.append(copy)
        return copy

    def arrived(copies):
        for copy in copies:
            copy.wait_recv()

    plane = [(dx, dy, 0) for dx in (-1, 0, 1) for dy in (-1, 0, 1) if dx or dy]
    bottom, top = here[2] == 0, here[2] == sizes[2] - 1
    barrier = pltpu.get_barrier_semaphore()

    def greet(offset):
        pl.semaphore_signal(barrier, inc=1, device_id=device(*offset), device_id_type=MESH)

    for offset in plane:
        greet(offset)
    greet((0, 0, -1))

    @pl.when(jnp.logical_not(top))
    def _():
        greet((0, 0, 1))

    loads = [
        pltpu.make_async_copy(vel_hbm, vel, load_sem.at[0]),
        pltpu.make_async_copy(vort_hbm, vort, load_sem.at[1]),
    ]
    for cp in loads:
        cp.start()

    wide = lax.broadcasted_iota(jnp.int32, (Y + 8, Z), 1)
    lane = lax.broadcasted_iota(jnp.int32, (Y, Z), 1)
    row = lax.broadcasted_iota(jnp.int32, (Y, Z), 0)
    cell = lane % W
    edge = (lane < 2) | (lane >= Z - 2)
    rim = (lane < 4) | (lane >= Z - 4)

    def faces(src, c):
        found = roll(src[c, 0], H + 4, 1)
        for x in range(1, X):
            found = jnp.where(lane >= H + W * x, roll(src[c, x], H + W * x + 4, 1), found)
        return found

    def spread_x(src, step, s, components=range(3)):
        for c in components:
            if s == 0:
                sx[step, 0, c, 0] = wgt[0, 0, 0] * src[c, 0]
                sx[step, 0, c, 1] = wgt[0, 1, 0] * src[c, 0] + wgt[0, 0, 1] * src[c, 1]
            else:
                sx[step, 1, c, 0] = (
                    wgt[0, 3, X - 1] * src[c, X - 1] + wgt[0, 4, X - 2] * src[c, X - 2])
                sx[step, 1, c, 1] = wgt[0, 4, X - 1] * src[c, X - 1]
            for t in range(2):
                sxy[step, s, t, c] = sx[step, s, c, :, pl.ds((Y - 2) * t, 2), :]

    def push_x(step, s, part=slice(None)):
        def piece(ref):
            return ref if part == slice(None) else ref.at[part]

        return [
            push(piece(sx.at[step, s]), piece(rx.at[step, s]), (SIDES[s], 0, 0))
        ] + [
            push(piece(sxy.at[step, s, t]), piece(rxy.at[step, s, t]), (SIDES[s], SIDES[t], 0))
            for t in range(2)
        ]

    def offer(first, values):
        for i, v in enumerate(values, first):
            ext[i, pl.ds(4, Y)] = v
            for t in range(2):
                ssy[t, i] = v[(Y - 4) * t:(Y - 4) * t + 4]

    def bundle(m):
        for s in range(2):
            found = None
            for j in range(4):
                moved = roll(ext[4 * m + j, pl.ds(4, Y)], H * (j - 1 - s), 1)
                found = moved if found is None else jnp.where(lane >= H * j, moved, found)
            ssx[s, m] = found
            for t in range(2):
                ssxy[s, t, m] = found[(Y - 4) * t:(Y - 4) * t + 4]

    def push_strip(bundles, units):
        copies = [
            push(ssx.at[s, bundles], rsx.at[s, bundles], (SIDES[s], 0, 0)) for s in (1, 0)
        ]
        copies += [
            push(ssxy.at[s, t, bundles], rsxy.at[s, t, bundles], (SIDES[s], SIDES[t], 0))
            for s in (1, 0) for t in range(2)
        ]
        copies += [
            push(ssy.at[t, units], rsy.at[t, units], (0, SIDES[t], 0)) for t in range(2)
        ]
        return copies

    def interior_x(src, step):
        for c in range(3):
            layers = []
            for x in range(X):
                total = None
                for a in range(-2, 3):
                    if 0 <= x - a < X:
                        term = wgt[0, a + 2, x - a] * src[c, x - a]
                        total = term if total is None else total + term
                layers.append(total)
            for x in range(X):
                cur[c, x] = layers[x]
                for t in range(2):
                    sy[step, t, c, x] = layers[x][(Y - 2) * t:(Y - 2) * t + 2]

    def push_y(step):
        return [push(sy.at[step, t], ry.at[step, t], (0, SIDES[t], 0)) for t in range(2)]

    def put_weights(k):
        for x in range(X):
            for a, w in enumerate(weights(vel[k, x])):
                if k == 1:
                    w = inside(w, a - 2, row, Y)
                if k == 2:
                    w = inside(w, a - 2, lane, Z)
                wgt[k, a, x] = w

    def ends(total, low, high, w):
        near = w[0] * low
        first = w[1] * low + jnp.concatenate([near[1:2], jnp.zeros_like(near[:1])], 0)
        near = w[2] * high
        last = w[3] * high + jnp.concatenate([jnp.zeros_like(near[:1]), near[0:1]], 0)
        gap = jnp.zeros((Y - 4, Z), jnp.float32)
        return total + jnp.concatenate([first, gap, last], 0)

    def pass_yz(step, x):
        after = []
        for c in range(3):
            v = cur[c, x]
            low, high = ry[step, 1, c, x], ry[step, 0, c, x]
            for s, i in ((1, x), (0, x - X + 2)):
                if 0 <= i < 2:
                    v = v + rx[step, s, c, i]
                    low = low + rxy[step, s, 1, c, i]
                    high = high + rxy[step, s, 0, c, i]
            total = wgt[1, 2, x] * v
            for a in (-2, -1, 1, 2):
                total = total + roll(wgt[1, a + 2, x] * v, a, 0)
            v = ends(total, low, high, [wgt_y[i, x] for i in range(4)])
            if step > 0:
                v = jnp.where(edge, 0.0, v)
            total = wgt[2, 2, x] * v
            for a in (-2, -1, 1, 2):
                total = total + roll(wgt[2, a + 2, x] * v, a, 1)
            after.append(total)
        return after

    def stretch(v, steepness):
        total = []
        for i in range(3):
            t = v[i]
            for j in range(3):
                t = t + v[j] * steepness(j, i)
            total.append(t)
        return total

    def passes(values, w, axes):
        for k, axis, size in axes:
            total = w(k, 2) * values
            for a in (-2, -1, 1, 2):
                total = total + roll(w(k, a + 2) * values, size * a, axis)
            values = total
        return values

    def slope_rows(v, axis, n=1):
        near = roll(v, -n, axis) - roll(v, n, axis)
        return scale * (8.0 * near - (roll(v, -2 * n, axis) - roll(v, 2 * n, axis)))

    def slope_ends(dst, v, low, high):
        top, end = v[0:4], v[Y - 4:Y]
        dst[0:1] = scale * (8.0 * (top[1:2] - low[1:2]) - (top[2:3] - low[0:1]))
        dst[1:2] = scale * (8.0 * (top[2:3] - top[0:1]) - (top[3:4] - low[1:2]))
        dst[Y - 2:Y - 1] = scale * (8.0 * (end[3:4] - end[1:2]) - (high[0:1] - end[0:1]))
        dst[Y - 1:Y] = scale * (8.0 * (high[0:1] - end[2:3]) - (high[1:2] - end[1:2]))

    def slope_x(layers, components=range(3)):
        for c in components:
            def layer(x):
                if x < 0:
                    return rvx[1, c, x + 2]
                if x >= X:
                    return rvx[0, c, x - X]
                return vel[c, x]
            for x in layers:
                slope[0, c, x] = scale * (
                    8.0 * (layer(x + 1) - layer(x - 1)) - (layer(x + 2) - layer(x - 2)))

    loads[0].wait()
    put_weights(0)
    loads[1].wait()
    own = [faces(vort, c) for c in range(3)] + [faces(vel, c) for c in range(3)]
    middle = (lane >= H) & (lane < Z - H)
    for m in range(3):
        sz[m] = jnp.where(middle, own[2 * m], roll(own[2 * m + 1], 2 * H, 1))
    for s in (1, 0):
        spread_x(vort, 0, s)
    for t in range(2):
        svy[t] = vel[:, :, pl.ds((Y - 2) * t, 2), :]
    pl.semaphore_wait(barrier, len(plane) + 1 + jnp.where(bottom, 0, 1))

    @pl.when(top)
    def _():
        pl.semaphore_signal(ready, inc=1, device_id=device(0, 0, 1), device_id_type=MESH)

    z_up = push(sz, rz.at[1], (0, 0, 1))
    z_down = push(sz, rz.at[0], (0, 0, -1), start=False)

    @pl.when(jnp.logical_not(bottom))
    def _():
        z_down.start()

    from_x, vel_x = {}, {}
    for s in (1, 0):
        from_x[s] = push_x(0, s)
        near = pl.ds((X - 2) * s, 2)
        if s:
            vel_x[s] = [push(vel.at[:, near], rvx.at[s], (SIDES[s], 0, 0))]
        else:
            vel_x[s] = [
                push(vel.at[c, near], rvx.at[s, c], (SIDES[s], 0, 0)) for c in range(3)
            ]
    vel_y = [push(svy.at[t], rvy.at[t], (0, SIDES[t], 0)) for t in range(2)]
    interior_x(vort, 0)
    from_y = push_y(0)
    offer(0, own)
    bundle(0)
    from_strip = push_strip(pl.ds(0, 1), pl.ds(0, 6))
    put_weights(1)
    put_weights(2)
    for c in range(3):
        for x in range(X):
            slope[1, c, x] = slope_rows(vel[c, x], 0)
            slope[2, c, x] = slope_rows(vel[c, x], 1)
    slope_x(range(2, X - 2))
    arrived(vel_y)
    for x in range(X):
        low, high = weights(rvy[1, 1, x]), weights(rvy[0, 1, x])
        for i, w in enumerate((low[3], low[4], high[1], high[0])):
            wgt_y[i, x] = w
    for c in range(3):
        for x in range(X):
            slope_ends(slope.at[1, c, x], vel[c, x], rvy[1, c, x], rvy[0, c, x])

    @pl.when(bottom)
    def _():
        pl.semaphore_wait(ready, 1)
        z_down.start()

    def advance(layers):
        for x in layers:
            v = stretch(pass_yz(0, x), lambda j, i: slope[j, i, x])
            for c in range(3):
                cur[c, x] = v[c]

    arrived([z_up, z_down])
    beyond = []
    for i in range(6):
        below, above = [roll(rz[s, i // 2], 2 * H * (i % 2), 1) for s in (1, 0)]
        beyond.append(jnp.where(cell < 4, below, above))
    offer(6, beyond)
    bundle(1)
    bundle(2)
    from_strip += push_strip(pl.ds(1, 2), pl.ds(6, 6))

    arrived(from_y)
    advance(range(2, X - 2))
    arrived(from_x[1] + vel_x[1])
    slope_x([0, 1])
    advance([0, 1])
    spread_x(cur, 1, 0)
    onward = {0: push_x(1, 0), 1: []}

    arrived(from_x[0])
    rest, along = {}, {}
    for x in (X - 2, X - 1):
        v = pass_yz(0, x)
        along[x] = v[0]
        rest[x] = [v[i] + v[1] * slope[1, i, x] + v[2] * slope[2, i, x] for i in range(3)]
    for c in range(3):
        arrived([vel_x[0][c]])
        slope_x([X - 2, X - 1], [c])
        for x in (X - 2, X - 1):
            cur[c, x] = rest[x][c] + along[x] * slope[0, c, x]
        spread_x(cur, 1, 1, [c])
        onward[1] += push_x(1, 1, c)
    interior_x(cur, 1)
    from_y = push_y(1)

    arrived(from_strip)
    tip = lane[:8]
    for i in range(12):
        m, j = divmod(i, 4)
        below, above = roll(rsx[1, m], -H * j, 1), roll(rsx[0, m], -H * (j + 1), 1)
        v = ext[i, pl.ds(4, Y)]
        ext[i, pl.ds(4, Y)] = jnp.where(lane < H, below, jnp.where(lane >= Z - H, above, v))
        below, above = [
            roll(jnp.concatenate([rsxy[s, 1, m], rsxy[s, 0, m]], 0), -H * (j + 1 - s), 1)
            for s in (1, 0)
        ]
        v = jnp.concatenate([rsy[1, i], rsy[0, i]], 0)
        v = jnp.where(tip < H, below, jnp.where(tip >= Z - H, above, v))
        ext[i, pl.ds(0, 4)] = v[0:4]
        ext[i, pl.ds(Y + 4, 4)] = v[4:8]
    inner = wide % W
    held = (inner >= 2) & (inner < 6)
    for i in range(6):
        pair[i, 0] = jnp.where(inner < 4, ext[6 + i], ext[i])
        pair[i, 1] = jnp.where(inner < 4, ext[i], ext[6 + i])
    for k in range(3):
        for a, w in enumerate(weights(pair[3 + k])):
            wgt_s[k, a] = w
    for c in range(3):
        v = pair[3 + c]
        for k, (axis, n) in enumerate(((2, W), (1, 1), (2, 1))):
            slope_s[k, c] = slope_rows(v, axis, n)

    def w(k, a):
        return wgt_s[k, a]

    in_x, in_y, in_z = (0, 2, W), (1, 1, 1), (2, 2, 1)
    v = [passes(pair[c], w, (in_x, in_y, in_z)) for c in range(3)]
    v = stretch(v, lambda j, i: slope_s[j, i])
    v = [passes(u, w, (in_x, in_y)) for u in v]
    v = [passes(jnp.where(held, u, 0.0), w, (in_z,)) for u in v]
    reach = [jnp.where(cell >= 4, u[0, 4:Y + 4], u[1, 4:Y + 4]) for u in v]
    for c in range(3):
        steep = jnp.where(
            cell >= 4, slope_s[2, c, 0, pl.ds(4, Y)], slope_s[2, c, 1, pl.ds(4, Y)])
        for x in range(X):
            slope[2, c, x] = jnp.where(edge, roll(steep, -(H + W * x + 4), 1), slope[2, c, x])

    def settle(layers):
        for x in layers:
            v = [
                u + jnp.where(rim, roll(reach[c], -(H + W * x + 4), 1), 0.0)
                for c, u in enumerate(pass_yz(1, x))
            ]
            v = stretch(v, lambda j, i: slope[j, i, x])
            for c in range(3):
                out[c, x] = v[c]

    arrived(from_y)
    settle(range(2, X - 2))
    for s, layers in ((0, [X - 2, X - 1]), (1, [0, 1])):
        arrived(onward[s])
        settle(layers)
    assert len(pushed) == COPIES
    for copy in pushed:
        copy.wait_send()


def solution(mesh):
    sizes = [mesh.shape[a] for a in AXES]

    def local(vort, vel):
        _, X, Y, Z = vort.shape
        S = SUBSTEPS

        def V(*shape):
            return pltpu.VMEM(shape, jnp.float32)

        return pl.pallas_call(
            functools.partial(body, sizes),
            out_shape=V(*vort.shape),
            in_specs=[pl.BlockSpec(memory_space=pl.ANY)] * 2,
            out_specs=pl.BlockSpec(memory_space=pltpu.VMEM),
            scratch_shapes=[
                V(3, X, Y, Z), V(3, X, Y, Z),
                V(3, 5, X, Y, Z), V(4, X, 2, Z), V(3, 3, X, Y, Z), V(3, X, Y, Z),
                V(12, Y + 8, Z), V(6, 2, Y + 8, Z), V(3, 5, 2, Y + 8, Z), V(3, 3, 2, Y + 8, Z),
                V(S, 2, 3, 2, Y, Z), V(S, 2, 3, 2, Y, Z),
                V(S, 2, 3, X, 2, Z), V(S, 2, 3, X, 2, Z),
                V(S, 2, 2, 3, 2, 2, Z), V(S, 2, 2, 3, 2, 2, Z),
                V(2, 3, 2, Y, Z),
                V(2, 3, X, 2, Z), V(2, 3, X, 2, Z),
                V(3, Y, Z), V(2, 3, Y, Z),
                V(2, 3, Y, Z), V(2, 3, Y, Z),
                V(2, 12, 4, Z), V(2, 12, 4, Z),
                V(2, 2, 3, 4, Z), V(2, 2, 3, 4, Z),
                pltpu.SemaphoreType.DMA((COPIES,)),
                pltpu.SemaphoreType.DMA((COPIES,)),
                pltpu.SemaphoreType.DMA((2,)),
                pltpu.SemaphoreType.REGULAR,
            ],
            compiler_params=pltpu.CompilerParams(collective_id=0, has_side_effects=True),
        )(vort, vel)

    placed = P(None, *AXES)
    return jax.shard_map(
        local, mesh=mesh, in_specs=(placed, placed), out_specs=placed, check_vma=False
    )
```

```python
import functools
import math

import jax
import jax.numpy as jnp
from jax import lax
from jax.experimental import pallas as pl
from jax.experimental.pallas import tpu as pltpu
from jax.sharding import PartitionSpec as P

SUBSTEPS = 2
TIME_STEP = 0.5
AXES = ("gx", "gy", "gz")
MESH = pl.DeviceIdType.MESH
SIDES = (-1, 1)
GROUPS = 12


def roll(values, shift, axis):
    shift %= values.shape[axis]
    return pltpu.roll(values, shift, axis) if shift else values


def weights(velocity):
    d = TIME_STEP * velocity
    s = jnp.abs(d)
    t = 1.0 - s
    positive = d > 0.0
    centre = 1.0 + s * s * (1.5 * s - 2.5)
    toward = 1.0 + t * t * (1.5 * t - 2.5)
    away = -0.5 * s * t * t
    beyond = -0.5 * s * s * t
    return (
        jnp.where(positive, 0.0, beyond),
        jnp.where(positive, away, toward),
        centre,
        jnp.where(positive, toward, away),
        jnp.where(positive, beyond, 0.0),
    )


def inside(w, a, index, extent):
    if a == 0:
        return w
    return jnp.where(index < extent - a if a > 0 else index >= -a, w, 0.0)


def body(
    sizes, vort_hbm, vel_hbm, out, vort, vel, wgt, wgt_y, slope, cur,
    ext, pair, wgt_s, slope_s,
    sx, rx, sy, ry, sxy, rxy, rvx, svy, rvy, sz, rz, ssx, rsx, ssy, rsy, ssxy, rsxy,
    total, send_sem, recv_sem, load_sem, ready,
):
    _, X, Y, Z = vort.shape
    W = 8
    H = 4 * W
    assert (X + 8) * W == Z and 2 * H + X * W == Z and Y >= 8
    scale = TIME_STEP / 12.0
    here = [lax.axis_index(a) for a in AXES]

    def device(*offset):
        return tuple(
            here[k] if not d else lax.rem(here[k] + (d % sizes[k]), sizes[k])
            for k, d in enumerate(offset)
        )

    rows = {}

    def push(src, dst, offset, group, start=True):
        rows.setdefault(group, 0)
        rows[group] += math.prod(src.shape[:-1])
        copy = pltpu.make_async_remote_copy(
            src_ref=src, dst_ref=dst, send_sem=send_sem.at[0],
            recv_sem=recv_sem.at[list(rows).index(group)],
            device_id=device(*offset), device_id_type=MESH,
        )
        if start:
            copy.start()
        return copy

    def tally(n, group=0):
        some = total.at[pl.ds(0, n)]
        return pltpu.make_async_remote_copy(
            src_ref=some, dst_ref=some, send_sem=send_sem.at[0], recv_sem=recv_sem.at[group],
            device_id=device(1, 0, 0), device_id_type=MESH,
        )

    def arrived(group):
        tally(rows[group], list(rows).index(group)).wait_recv()

    plane = [(dx, dy, 0) for dx in (-1, 0, 1) for dy in (-1, 0, 1) if dx or dy]
    bottom, top = here[2] == 0, here[2] == sizes[2] - 1
    barrier = pltpu.get_barrier_semaphore()

    def greet(offset):
        pl.semaphore_signal(barrier, inc=1, device_id=device(*offset), device_id_type=MESH)

    for offset in plane:
        greet(offset)
    greet((0, 0, -1))

    @pl.when(jnp.logical_not(top))
    def _():
        greet((0, 0, 1))

    loads = [
        pltpu.make_async_copy(vel_hbm, vel, load_sem.at[0]),
        pltpu.make_async_copy(vort_hbm, vort, load_sem.at[1]),
    ]
    for cp in loads:
        cp.start()

    wide = lax.broadcasted_iota(jnp.int32, (Y + 8, Z), 1)
    lane = lax.broadcasted_iota(jnp.int32, (Y, Z), 1)
    row = lax.broadcasted_iota(jnp.int32, (Y, Z), 0)
    cell = lane % W
    edge = (lane < 2) | (lane >= Z - 2)
    rim = (lane < 4) | (lane >= Z - 4)

    def faces(src, c):
        found = roll(src[c, 0], H + 4, 1)
        for x in range(1, X):
            found = jnp.where(lane >= H + W * x, roll(src[c, x], H + W * x + 4, 1), found)
        return found

    def spread_x(src, step, s, components=range(3)):
        for c in components:
            if s == 0:
                sx[step, 0, c, 0] = wgt[0, 0, 0] * src[c, 0]
                sx[step, 0, c, 1] = wgt[0, 1, 0] * src[c, 0] + wgt[0, 0, 1] * src[c, 1]
            else:
                sx[step, 1, c, 0] = (
                    wgt[0, 3, X - 1] * src[c, X - 1] + wgt[0, 4, X - 2] * src[c, X - 2])
                sx[step, 1, c, 1] = wgt[0, 4, X - 1] * src[c, X - 1]
            for t in range(2):
                sxy[step, s, t, c] = sx[step, s, c, :, pl.ds((Y - 2) * t, 2), :]

    def push_x(step, s, group, part=slice(None)):
        def piece(ref):
            return ref if part == slice(None) else ref.at[part]

        push(piece(sx.at[step, s]), piece(rx.at[step, s]), (SIDES[s], 0, 0), group)
        for t in range(2):
            push(
                piece(sxy.at[step, s, t]), piece(rxy.at[step, s, t]), (SIDES[s], SIDES[t], 0),
                group)

    def offer(first, values):
        for i, v in enumerate(values, first):
            ext[i, pl.ds(4, Y)] = v
            for t in range(2):
                ssy[t, i] = v[(Y - 4) * t:(Y - 4) * t + 4]

    def bundle(m):
        for s in range(2):
            found = None
            for j in range(4):
                moved = roll(ext[4 * m + j, pl.ds(4, Y)], H * (j - 1 - s), 1)
                found = moved if found is None else jnp.where(lane >= H * j, moved, found)
            ssx[s, m] = found
            for t in range(2):
                ssxy[s, t, m] = found[(Y - 4) * t:(Y - 4) * t + 4]

    def push_strip(bundles, units):
        for s in (1, 0):
            push(ssx.at[s, bundles], rsx.at[s, bundles], (SIDES[s], 0, 0), "strip")
            for t in range(2):
                push(
                    ssxy.at[s, t, bundles], rsxy.at[s, t, bundles], (SIDES[s], SIDES[t], 0),
                    "strip")
        for t in range(2):
            push(ssy.at[t, units], rsy.at[t, units], (0, SIDES[t], 0), "strip")

    def interior_x(src, step):
        for c in range(3):
            layers = []
            for x in range(X):
                total = None
                for a in range(-2, 3):
                    if 0 <= x - a < X:
                        term = wgt[0, a + 2, x - a] * src[c, x - a]
                        total = term if total is None else total + term
                layers.append(total)
            for x in range(X):
                cur[c, x] = layers[x]
                for t in range(2):
                    sy[step, t, c, x] = layers[x][(Y - 2) * t:(Y - 2) * t + 2]

    def push_y(step):
        for t in range(2):
            push(sy.at[step, t], ry.at[step, t], (0, SIDES[t], 0), f"y{step}")

    def put_weights(k, layers):
        for x in layers:
            for a, w in enumerate(weights(vel[k, x])):
                if k == 1:
                    w = inside(w, a - 2, row, Y)
                if k == 2:
                    w = inside(w, a - 2, lane, Z)
                wgt[k, a, x] = w

    def ends(total, low, high, w):
        near = w[0] * low
        first = w[1] * low + jnp.concatenate([near[1:2], jnp.zeros_like(near[:1])], 0)
        near = w[2] * high
        last = w[3] * high + jnp.concatenate([jnp.zeros_like(near[:1]), near[0:1]], 0)
        gap = jnp.zeros((Y - 4, Z), jnp.float32)
        return total + jnp.concatenate([first, gap, last], 0)

    def pass_yz(step, x):
        after = []
        for c in range(3):
            v = cur[c, x]
            low, high = ry[step, 1, c, x], ry[step, 0, c, x]
            for s, i in ((1, x), (0, x - X + 2)):
                if 0 <= i < 2:
                    v = v + rx[step, s, c, i]
                    low = low + rxy[step, s, 1, c, i]
                    high = high + rxy[step, s, 0, c, i]
            total = wgt[1, 2, x] * v
            for a in (-2, -1, 1, 2):
                total = total + roll(wgt[1, a + 2, x] * v, a, 0)
            v = ends(total, low, high, [wgt_y[i, x] for i in range(4)])
            if step > 0:
                v = jnp.where(edge, 0.0, v)
            total = wgt[2, 2, x] * v
            for a in (-2, -1, 1, 2):
                total = total + roll(wgt[2, a + 2, x] * v, a, 1)
            after.append(total)
        return after

    def stretch(v, steepness):
        total = []
        for i in range(3):
            t = v[i]
            for j in range(3):
                t = t + v[j] * steepness(j, i)
            total.append(t)
        return total

    def passes(values, w, axes):
        for k, axis, size in axes:
            total = w(k, 2) * values
            for a in (-2, -1, 1, 2):
                total = total + roll(w(k, a + 2) * values, size * a, axis)
            values = total
        return values

    def slope_rows(v, axis, n=1):
        near = roll(v, -n, axis) - roll(v, n, axis)
        return scale * (8.0 * near - (roll(v, -2 * n, axis) - roll(v, 2 * n, axis)))

    def slope_ends(dst, v, low, high):
        top, end = v[0:4], v[Y - 4:Y]
        dst[0:1] = scale * (8.0 * (top[1:2] - low[1:2]) - (top[2:3] - low[0:1]))
        dst[1:2] = scale * (8.0 * (top[2:3] - top[0:1]) - (top[3:4] - low[1:2]))
        dst[Y - 2:Y - 1] = scale * (8.0 * (end[3:4] - end[1:2]) - (high[0:1] - end[0:1]))
        dst[Y - 1:Y] = scale * (8.0 * (high[0:1] - end[2:3]) - (high[1:2] - end[1:2]))

    def slope_x(layers, components=range(3)):
        for c in components:
            def layer(x):
                if x < 0:
                    return rvx[1, c, x + 2]
                if x >= X:
                    return rvx[0, c, x - X]
                return vel[c, x]
            for x in layers:
                slope[0, c, x] = scale * (
                    8.0 * (layer(x + 1) - layer(x - 1)) - (layer(x + 2) - layer(x - 2)))

    loads[0].wait()
    put_weights(0, [0, 1, X - 2, X - 1])
    loads[1].wait()
    for s in (1, 0):
        spread_x(vort, 0, s)
    pl.semaphore_wait(barrier, len(plane) + 1 + jnp.where(bottom, 0, 1))

    @pl.when(top)
    def _():
        pl.semaphore_signal(ready, inc=1, device_id=device(0, 0, 1), device_id_type=MESH)

    for s in (1, 0):
        push_x(0, s, f"x{s}")
        near = pl.ds((X - 2) * s, 2)
        if s:
            push(vel.at[:, near], rvx.at[s], (SIDES[s], 0, 0), "x1")
        else:
            for c in range(3):
                push(vel.at[c, near], rvx.at[s, c], (SIDES[s], 0, 0), f"vel{c}")
    own = [faces(vort, c) for c in range(3)] + [faces(vel, c) for c in range(3)]
    middle = (lane >= H) & (lane < Z - H)
    for m in range(3):
        sz[m] = jnp.where(middle, own[2 * m], roll(own[2 * m + 1], 2 * H, 1))
    push(sz, rz.at[1], (0, 0, 1), "z")
    z_down = push(sz, rz.at[0], (0, 0, -1), "z", start=False)

    @pl.when(jnp.logical_not(bottom))
    def _():
        z_down.start()

    for t in range(2):
        svy[t] = vel[:, :, pl.ds((Y - 2) * t, 2), :]
        push(svy.at[t], rvy.at[t], (0, SIDES[t], 0), "vel_y")
    put_weights(0, range(2, X - 2))
    interior_x(vort, 0)
    push_y(0)
    offer(0, own)
    bundle(0)
    push_strip(pl.ds(0, 1), pl.ds(0, 6))
    put_weights(1, range(X))
    put_weights(2, range(X))
    for c in range(3):
        for x in range(X):
            slope[1, c, x] = slope_rows(vel[c, x], 0)
            slope[2, c, x] = slope_rows(vel[c, x], 1)
    slope_x(range(2, X - 2))
    arrived("vel_y")
    for x in range(X):
        low, high = weights(rvy[1, 1, x]), weights(rvy[0, 1, x])
        for i, w in enumerate((low[3], low[4], high[1], high[0])):
            wgt_y[i, x] = w
    for c in range(3):
        for x in range(X):
            slope_ends(slope.at[1, c, x], vel[c, x], rvy[1, c, x], rvy[0, c, x])

    @pl.when(bottom)
    def _():
        pl.semaphore_wait(ready, 1)
        z_down.start()

    def advance(layers):
        for x in layers:
            v = stretch(pass_yz(0, x), lambda j, i: slope[j, i, x])
            for c in range(3):
                cur[c, x] = v[c]

    arrived("z")
    beyond = []
    for i in range(6):
        below, above = [roll(rz[s, i // 2], 2 * H * (i % 2), 1) for s in (1, 0)]
        beyond.append(jnp.where(cell < 4, below, above))
    offer(6, beyond)
    bundle(1)
    bundle(2)
    push_strip(pl.ds(1, 2), pl.ds(6, 6))

    arrived("y0")
    advance(range(2, X - 2))
    arrived("x1")
    slope_x([0, 1])
    advance([0, 1])
    spread_x(cur, 1, 0)
    push_x(1, 0, "x0 again")

    arrived("x0")
    rest, along = {}, {}
    for x in (X - 2, X - 1):
        v = pass_yz(0, x)
        along[x] = v[0]
        rest[x] = [v[i] + v[1] * slope[1, i, x] + v[2] * slope[2, i, x] for i in range(3)]
    for c in range(3):
        arrived(f"vel{c}")
        slope_x([X - 2, X - 1], [c])
        for x in (X - 2, X - 1):
            cur[c, x] = rest[x][c] + along[x] * slope[0, c, x]
        spread_x(cur, 1, 1, [c])
        push_x(1, 1, "x1 again", c)
    interior_x(cur, 1)
    push_y(1)

    arrived("strip")
    tip = lane[:8]
    for i in range(12):
        m, j = divmod(i, 4)
        below, above = roll(rsx[1, m], -H * j, 1), roll(rsx[0, m], -H * (j + 1), 1)
        v = ext[i, pl.ds(4, Y)]
        ext[i, pl.ds(4, Y)] = jnp.where(lane < H, below, jnp.where(lane >= Z - H, above, v))
        below, above = [
            roll(jnp.concatenate([rsxy[s, 1, m], rsxy[s, 0, m]], 0), -H * (j + 1 - s), 1)
            for s in (1, 0)
        ]
        v = jnp.concatenate([rsy[1, i], rsy[0, i]], 0)
        v = jnp.where(tip < H, below, jnp.where(tip >= Z - H, above, v))
        ext[i, pl.ds(0, 4)] = v[0:4]
        ext[i, pl.ds(Y + 4, 4)] = v[4:8]
    inner = wide % W
    held = (inner >= 2) & (inner < 6)
    for i in range(6):
        pair[i, 0] = jnp.where(inner < 4, ext[6 + i], ext[i])
        pair[i, 1] = jnp.where(inner < 4, ext[i], ext[6 + i])
    for k in range(3):
        for a, w in enumerate(weights(pair[3 + k])):
            wgt_s[k, a] = w
    for c in range(3):
        v = pair[3 + c]
        for k, (axis, n) in enumerate(((2, W), (1, 1), (2, 1))):
            slope_s[k, c] = slope_rows(v, axis, n)

    def w(k, a):
        return wgt_s[k, a]

    in_x, in_y, in_z = (0, 2, W), (1, 1, 1), (2, 2, 1)
    v = [passes(pair[c], w, (in_x, in_y, in_z)) for c in range(3)]
    v = stretch(v, lambda j, i: slope_s[j, i])
    v = [passes(u, w, (in_x, in_y)) for u in v]
    v = [passes(jnp.where(held, u, 0.0), w, (in_z,)) for u in v]
    reach = [jnp.where(cell >= 4, u[0, 4:Y + 4], u[1, 4:Y + 4]) for u in v]
    for c in range(3):
        steep = jnp.where(
            cell >= 4, slope_s[2, c, 0, pl.ds(4, Y)], slope_s[2, c, 1, pl.ds(4, Y)])
        for x in range(X):
            slope[2, c, x] = jnp.where(edge, roll(steep, -(H + W * x + 4), 1), slope[2, c, x])

    def settle(layers):
        for x in layers:
            v = [
                u + jnp.where(rim, roll(reach[c], -(H + W * x + 4), 1), 0.0)
                for c, u in enumerate(pass_yz(1, x))
            ]
            v = stretch(v, lambda j, i: slope[j, i, x])
            for c in range(3):
                out[c, x] = v[c]

    arrived("y1")
    settle(range(2, X - 2))
    for s, layers in ((0, [X - 2, X - 1]), (1, [0, 1])):
        arrived(f"x{s} again")
        settle(layers)
    assert len(rows) == GROUPS and sum(rows.values()) == total.shape[0]
    tally(sum(rows.values())).wait_send()


def solution(mesh):
    sizes = [mesh.shape[a] for a in AXES]

    def local(vort, vel):
        _, X, Y, Z = vort.shape
        S = SUBSTEPS

        def V(*shape):
            return pltpu.VMEM(shape, jnp.float32)

        return pl.pallas_call(
            functools.partial(body, sizes),
            out_shape=V(*vort.shape),
            in_specs=[pl.BlockSpec(memory_space=pl.ANY)] * 2,
            out_specs=pl.BlockSpec(memory_space=pltpu.VMEM),
            scratch_shapes=[
                V(3, X, Y, Z), V(3, X, Y, Z),
                V(3, 5, X, Y, Z), V(4, X, 2, Z), V(3, 3, X, Y, Z), V(3, X, Y, Z),
                V(12, Y + 8, Z), V(6, 2, Y + 8, Z), V(3, 5, 2, Y + 8, Z), V(3, 3, 2, Y + 8, Z),
                V(S, 2, 3, 2, Y, Z), V(S, 2, 3, 2, Y, Z),
                V(S, 2, 3, X, 2, Z), V(S, 2, 3, X, 2, Z),
                V(S, 2, 2, 3, 2, 2, Z), V(S, 2, 2, 3, 2, 2, Z),
                V(2, 3, 2, Y, Z),
                V(2, 3, X, 2, Z), V(2, 3, X, 2, Z),
                V(3, Y, Z), V(2, 3, Y, Z),
                V(2, 3, Y, Z), V(2, 3, Y, Z),
                V(2, 12, 4, Z), V(2, 12, 4, Z),
                V(2, 2, 3, 4, Z), V(2, 2, 3, 4, Z),
                V(48 * Y + 36 * X + 240, 1, Z),
                pltpu.SemaphoreType.DMA((1,)),
                pltpu.SemaphoreType.DMA((GROUPS,)),
                pltpu.SemaphoreType.DMA((2,)),
                pltpu.SemaphoreType.REGULAR,
            ],
            compiler_params=pltpu.CompilerParams(collective_id=0, has_side_effects=True),
        )(vort, vel)

    placed = P(None, *AXES)
    return jax.shard_map(
        local, mesh=mesh, in_specs=(placed, placed), out_specs=placed, check_vma=False
    )
```

```python
import functools
import math

import jax
import jax.numpy as jnp
from jax import lax
from jax.experimental import pallas as pl
from jax.experimental.pallas import tpu as pltpu
from jax.sharding import PartitionSpec as P

SUBSTEPS = 2
TIME_STEP = 0.5
AXES = ("gx", "gy", "gz")
MESH = pl.DeviceIdType.MESH
SIDES = (-1, 1)
GROUPS = 14


def roll(values, shift, axis):
    shift %= values.shape[axis]
    return pltpu.roll(values, shift, axis) if shift else values


def weights(velocity):
    d = TIME_STEP * velocity
    s = jnp.abs(d)
    t = 1.0 - s
    positive = d > 0.0
    centre = 1.0 + s * s * (1.5 * s - 2.5)
    toward = 1.0 + t * t * (1.5 * t - 2.5)
    away = -0.5 * s * t * t
    beyond = -0.5 * s * s * t
    return (
        jnp.where(positive, 0.0, beyond),
        jnp.where(positive, away, toward),
        centre,
        jnp.where(positive, toward, away),
        jnp.where(positive, beyond, 0.0),
    )


def inside(w, a, index, extent):
    if a == 0:
        return w
    return jnp.where(index < extent - a if a > 0 else index >= -a, w, 0.0)


def body(
    sizes, vort_hbm, vel_hbm, out, vort, vel, wgt, wgt_y, slope, cur,
    ext, pair, wgt_s, slope_s,
    sx, rx, sy, ry, sxy, rxy, rvx, svy, rvy, sz, rz, ssx, rsx, ssy, rsy, ssxy, rsxy,
    total, send_sem, recv_sem, load_sem, ready,
):
    _, X, Y, Z = vort.shape
    W = 8
    H = 4 * W
    assert (X + 8) * W == Z and 2 * H + X * W == Z and Y >= 8
    scale = TIME_STEP / 12.0
    here = [lax.axis_index(a) for a in AXES]

    def device(*offset):
        return tuple(
            here[k] if not d else lax.rem(here[k] + (d % sizes[k]), sizes[k])
            for k, d in enumerate(offset)
        )

    rows = {}

    def push(src, dst, offset, group, start=True):
        rows.setdefault(group, 0)
        rows[group] += math.prod(src.shape[:-1])
        copy = pltpu.make_async_remote_copy(
            src_ref=src, dst_ref=dst, send_sem=send_sem.at[0],
            recv_sem=recv_sem.at[list(rows).index(group)],
            device_id=device(*offset), device_id_type=MESH,
        )
        if start:
            copy.start()
        return copy

    def tally(n, group=0):
        some = total.at[pl.ds(0, n)]
        return pltpu.make_async_remote_copy(
            src_ref=some, dst_ref=some, send_sem=send_sem.at[0], recv_sem=recv_sem.at[group],
            device_id=device(1, 0, 0), device_id_type=MESH,
        )

    def arrived(group):
        tally(rows[group], list(rows).index(group)).wait_recv()

    loads = [
        pltpu.make_async_copy(vel_hbm, vel, load_sem.at[0]),
        pltpu.make_async_copy(vort_hbm, vort, load_sem.at[1]),
    ]
    for cp in loads:
        cp.start()

    plane = [(dx, dy, 0) for dx in (-1, 0, 1) for dy in (-1, 0, 1) if dx or dy]
    bottom, top = here[2] == 0, here[2] == sizes[2] - 1
    barrier = pltpu.get_barrier_semaphore()

    def greet(offset):
        pl.semaphore_signal(barrier, inc=1, device_id=device(*offset), device_id_type=MESH)

    for offset in plane:
        greet(offset)
    greet((0, 0, -1))

    @pl.when(jnp.logical_not(top))
    def _():
        greet((0, 0, 1))

    wide = lax.broadcasted_iota(jnp.int32, (Y + 8, Z), 1)
    lane = lax.broadcasted_iota(jnp.int32, (Y, Z), 1)
    row = lax.broadcasted_iota(jnp.int32, (Y, Z), 0)
    cell = lane % W
    edge = (lane < 2) | (lane >= Z - 2)
    rim = (lane < 4) | (lane >= Z - 4)

    def faces(src, c):
        found = roll(src[c, 0], H + 4, 1)
        for x in range(1, X):
            found = jnp.where(lane >= H + W * x, roll(src[c, x], H + W * x + 4, 1), found)
        return found

    def spread_x(src, step, s, components=range(3)):
        for c in components:
            if s == 0:
                sx[step, 0, c, 0] = wgt[0, 0, 0] * src[c, 0]
                sx[step, 0, c, 1] = wgt[0, 1, 0] * src[c, 0] + wgt[0, 0, 1] * src[c, 1]
            else:
                sx[step, 1, c, 0] = (
                    wgt[0, 3, X - 1] * src[c, X - 1] + wgt[0, 4, X - 2] * src[c, X - 2])
                sx[step, 1, c, 1] = wgt[0, 4, X - 1] * src[c, X - 1]
            for t in range(2):
                sxy[step, s, t, c] = sx[step, s, c, :, pl.ds((Y - 2) * t, 2), :]

    def push_x(step, s, group, part=slice(None)):
        def piece(ref):
            return ref if part == slice(None) else ref.at[part]

        push(piece(sx.at[step, s]), piece(rx.at[step, s]), (SIDES[s], 0, 0), group)
        for t in range(2):
            push(
                piece(sxy.at[step, s, t]), piece(rxy.at[step, s, t]), (SIDES[s], SIDES[t], 0),
                group)

    def offer(first, values):
        for i, v in enumerate(values, first):
            ext[i, pl.ds(4, Y)] = v
            for t in range(2):
                ssy[t, i] = v[(Y - 4) * t:(Y - 4) * t + 4]

    def bundle(m):
        for s in range(2):
            found = None
            for j in range(4):
                moved = roll(ext[4 * m + j, pl.ds(4, Y)], H * (j - 1 - s), 1)
                found = moved if found is None else jnp.where(lane >= H * j, moved, found)
            ssx[s, m] = found
            for t in range(2):
                ssxy[s, t, m] = found[(Y - 4) * t:(Y - 4) * t + 4]

    def push_strip(bundles, units):
        for s in (1, 0):
            push(ssx.at[s, bundles], rsx.at[s, bundles], (SIDES[s], 0, 0), "strip")
            for t in range(2):
                push(
                    ssxy.at[s, t, bundles], rsxy.at[s, t, bundles], (SIDES[s], SIDES[t], 0),
                    "strip")
        for t in range(2):
            push(ssy.at[t, units], rsy.at[t, units], (0, SIDES[t], 0), "strip")

    def interior_x(src, step):
        for c in range(3):
            layers = []
            for x in range(X):
                total = None
                for a in range(-2, 3):
                    if 0 <= x - a < X:
                        term = wgt[0, a + 2, x - a] * src[c, x - a]
                        total = term if total is None else total + term
                layers.append(total)
            for x in range(X):
                cur[c, x] = layers[x]
                for t in range(2):
                    sy[step, t, c, x] = layers[x][(Y - 2) * t:(Y - 2) * t + 2]

    def push_y(step):
        for t in range(2):
            push(sy.at[step, t], ry.at[step, t], (0, SIDES[t], 0), f"y{step}")

    def put_weights(k, layers):
        for x in layers:
            for a, w in enumerate(weights(vel[k, x])):
                if k == 1:
                    w = inside(w, a - 2, row, Y)
                if k == 2:
                    w = inside(w, a - 2, lane, Z)
                wgt[k, a, x] = w

    def ends(total, low, high, w):
        near = w[0] * low
        first = w[1] * low + jnp.concatenate([near[1:2], jnp.zeros_like(near[:1])], 0)
        near = w[2] * high
        last = w[3] * high + jnp.concatenate([jnp.zeros_like(near[:1]), near[0:1]], 0)
        gap = jnp.zeros((Y - 4, Z), jnp.float32)
        return total + jnp.concatenate([first, gap, last], 0)

    def pass_yz(step, x, components=range(3)):
        after = []
        for c in components:
            v = cur[c, x]
            low, high = ry[step, 1, c, x], ry[step, 0, c, x]
            for s, i in ((1, x), (0, x - X + 2)):
                if 0 <= i < 2:
                    v = v + rx[step, s, c, i]
                    low = low + rxy[step, s, 1, c, i]
                    high = high + rxy[step, s, 0, c, i]
            total = wgt[1, 2, x] * v
            for a in (-2, -1, 1, 2):
                total = total + roll(wgt[1, a + 2, x] * v, a, 0)
            v = ends(total, low, high, [wgt_y[i, x] for i in range(4)])
            if step > 0:
                v = jnp.where(edge, 0.0, v)
            total = wgt[2, 2, x] * v
            for a in (-2, -1, 1, 2):
                total = total + roll(wgt[2, a + 2, x] * v, a, 1)
            after.append(total)
        return after

    def stretch(v, steepness):
        total = []
        for i in range(3):
            t = v[i]
            for j in range(3):
                t = t + v[j] * steepness(j, i)
            total.append(t)
        return total

    def passes(values, w, axes):
        for k, axis, size in axes:
            total = w(k, 2) * values
            for a in (-2, -1, 1, 2):
                total = total + roll(w(k, a + 2) * values, size * a, axis)
            values = total
        return values

    def slope_rows(v, axis, n=1):
        near = roll(v, -n, axis) - roll(v, n, axis)
        return scale * (8.0 * near - (roll(v, -2 * n, axis) - roll(v, 2 * n, axis)))

    def slope_ends(dst, v, low, high):
        top, end = v[0:4], v[Y - 4:Y]
        dst[0:1] = scale * (8.0 * (top[1:2] - low[1:2]) - (top[2:3] - low[0:1]))
        dst[1:2] = scale * (8.0 * (top[2:3] - top[0:1]) - (top[3:4] - low[1:2]))
        dst[Y - 2:Y - 1] = scale * (8.0 * (end[3:4] - end[1:2]) - (high[0:1] - end[0:1]))
        dst[Y - 1:Y] = scale * (8.0 * (high[0:1] - end[2:3]) - (high[1:2] - end[1:2]))

    def slope_x(layers, components=range(3)):
        for c in components:
            def layer(x):
                if x < 0:
                    return rvx[1, c, x + 2]
                if x >= X:
                    return rvx[0, c, x - X]
                return vel[c, x]
            for x in layers:
                slope[0, c, x] = scale * (
                    8.0 * (layer(x + 1) - layer(x - 1)) - (layer(x + 2) - layer(x - 2)))

    loads[0].wait()
    put_weights(0, [0, 1, X - 2, X - 1])
    loads[1].wait()
    for s in (1, 0):
        spread_x(vort, 0, s)
    own = [faces(vort, c) for c in range(3)] + [faces(vel, c) for c in range(3)]
    middle = (lane >= H) & (lane < Z - H)
    for m in range(2):
        for up in range(2):
            found = None
            for j, v in enumerate(own[4 * m:4 * m + 4]):
                h, late = j % 2, j // 2
                moved = roll(v, 2 * H * h + 4 * (late - 1 + up), 1)
                spot = middle == (h == 0)
                if late:
                    spot = spot & (cell >= 4)
                found = moved if found is None else jnp.where(spot, moved, found)
            sz[up, m] = found
    pl.semaphore_wait(barrier, len(plane) + 1 + jnp.where(bottom, 0, 1))

    @pl.when(top)
    def _():
        pl.semaphore_signal(ready, inc=1, device_id=device(0, 0, 1), device_id_type=MESH)

    push(sz.at[1], rz.at[1], (0, 0, 1), "z")
    z_down = push(sz.at[0], rz.at[0], (0, 0, -1), "z", start=False)

    @pl.when(jnp.logical_not(bottom))
    def _():
        z_down.start()

    for s in (1, 0):
        push_x(0, s, f"x{s}")
        near = pl.ds((X - 2) * s, 2)
        if s:
            push(vel.at[:, near], rvx.at[s], (SIDES[s], 0, 0), "x1")
        else:
            for c in range(3):
                push(vel.at[c, near], rvx.at[s, c], (SIDES[s], 0, 0), f"vel{c}")
    for t in range(2):
        svy[t] = vel[:, :, pl.ds((Y - 2) * t, 2), :]
        push(svy.at[t], rvy.at[t], (0, SIDES[t], 0), "vel_y")
    put_weights(0, range(2, X - 2))
    interior_x(vort, 0)
    push_y(0)
    offer(0, own)
    bundle(0)
    push_strip(pl.ds(0, 1), pl.ds(0, 6))
    put_weights(1, range(X))
    put_weights(2, range(X))
    for c in range(3):
        for x in range(X):
            slope[1, c, x] = slope_rows(vel[c, x], 0)
            slope[2, c, x] = slope_rows(vel[c, x], 1)
    slope_x(range(2, X - 2))
    arrived("vel_y")
    for x in range(X):
        low, high = weights(rvy[1, 1, x]), weights(rvy[0, 1, x])
        for i, w in enumerate((low[3], low[4], high[1], high[0])):
            wgt_y[i, x] = w
    for c in range(3):
        for x in range(X):
            slope_ends(slope.at[1, c, x], vel[c, x], rvy[1, c, x], rvy[0, c, x])

    @pl.when(bottom)
    def _():
        pl.semaphore_wait(ready, 1)
        z_down.start()

    def advance(layers):
        for x in layers:
            v = stretch(pass_yz(0, x), lambda j, i: slope[j, i, x])
            for c in range(3):
                cur[c, x] = v[c]

    arrived("z")
    beyond = []
    for i in range(6):
        h, late = i % 2, i % 4 // 2
        below = roll(rz[1, i // 4], 2 * H * h - 4 * late, 1)
        above = roll(rz[0, i // 4], 2 * H * h + 4 - 4 * late, 1)
        beyond.append(jnp.where(cell < 4, below, above))
    offer(6, beyond)
    bundle(1)
    bundle(2)
    push_strip(pl.ds(1, 2), pl.ds(6, 6))

    arrived("y0")
    advance(range(2, X - 2))
    arrived("x1")
    slope_x([0, 1])
    advance([0, 1])
    spread_x(cur, 1, 0)
    push_x(1, 0, "x0 again")

    arrived("x0")
    rest, along = {}, {}
    for x in (X - 2, X - 1):
        v = pass_yz(0, x)
        along[x] = v[0]
        rest[x] = [v[i] + v[1] * slope[1, i, x] + v[2] * slope[2, i, x] for i in range(3)]
    for c in range(3):
        arrived(f"vel{c}")
        slope_x([X - 2, X - 1], [c])
        for x in (X - 2, X - 1):
            cur[c, x] = rest[x][c] + along[x] * slope[0, c, x]
        spread_x(cur, 1, 1, [c])
        push_x(1, 1, f"x1 again{c}", c)
    interior_x(cur, 1)
    push_y(1)

    arrived("strip")
    tip = lane[:8]
    for i in range(12):
        m, j = divmod(i, 4)
        below, above = roll(rsx[1, m], -H * j, 1), roll(rsx[0, m], -H * (j + 1), 1)
        v = ext[i, pl.ds(4, Y)]
        ext[i, pl.ds(4, Y)] = jnp.where(lane < H, below, jnp.where(lane >= Z - H, above, v))
        below, above = [
            roll(jnp.concatenate([rsxy[s, 1, m], rsxy[s, 0, m]], 0), -H * (j + 1 - s), 1)
            for s in (1, 0)
        ]
        v = jnp.concatenate([rsy[1, i], rsy[0, i]], 0)
        v = jnp.where(tip < H, below, jnp.where(tip >= Z - H, above, v))
        ext[i, pl.ds(0, 4)] = v[0:4]
        ext[i, pl.ds(Y + 4, 4)] = v[4:8]
    inner = wide % W
    held = (inner >= 2) & (inner < 6)
    for i in range(6):
        pair[i, 0] = jnp.where(inner < 4, ext[6 + i], ext[i])
        pair[i, 1] = jnp.where(inner < 4, ext[i], ext[6 + i])
    for k in range(3):
        for a, w in enumerate(weights(pair[3 + k])):
            wgt_s[k, a] = w
    for c in range(3):
        v = pair[3 + c]
        for k, (axis, n) in enumerate(((2, W), (1, 1), (2, 1))):
            slope_s[k, c] = slope_rows(v, axis, n)

    def w(k, a):
        return wgt_s[k, a]

    in_x, in_y, in_z = (0, 2, W), (1, 1, 1), (2, 2, 1)
    v = [passes(pair[c], w, (in_x, in_y, in_z)) for c in range(3)]
    v = stretch(v, lambda j, i: slope_s[j, i])
    v = [passes(u, w, (in_x, in_y)) for u in v]
    v = [passes(jnp.where(held, u, 0.0), w, (in_z,)) for u in v]
    reach = [jnp.where(cell >= 4, u[0, 4:Y + 4], u[1, 4:Y + 4]) for u in v]
    for c in range(3):
        steep = jnp.where(
            cell >= 4, slope_s[2, c, 0, pl.ds(4, Y)], slope_s[2, c, 1, pl.ds(4, Y)])
        for x in range(X):
            slope[2, c, x] = jnp.where(edge, roll(steep, -(H + W * x + 4), 1), slope[2, c, x])

    def settle(layers):
        for x in layers:
            v = [
                u + jnp.where(rim, roll(reach[c], -(H + W * x + 4), 1), 0.0)
                for c, u in enumerate(pass_yz(1, x))
            ]
            v = stretch(v, lambda j, i: slope[j, i, x])
            for c in range(3):
                out[c, x] = v[c]

    arrived("y1")
    settle(range(2, X - 2))
    arrived("x0 again")
    settle([X - 2, X - 1])
    late = {0: [], 1: []}
    for c in range(3):
        arrived(f"x1 again{c}")
        for x in (0, 1):
            late[x].append(
                pass_yz(1, x, [c])[0]
                + jnp.where(rim, roll(reach[c], -(H + W * x + 4), 1), 0.0))
    for x in (0, 1):
        v = stretch(late[x], lambda j, i: slope[j, i, x])
        for c in range(3):
            out[c, x] = v[c]
    assert len(rows) == GROUPS and sum(rows.values()) == total.shape[0]
    tally(sum(rows.values())).wait_send()


def solution(mesh):
    sizes = [mesh.shape[a] for a in AXES]

    def local(vort, vel):
        _, X, Y, Z = vort.shape
        S = SUBSTEPS

        def V(*shape):
            return pltpu.VMEM(shape, jnp.float32)

        return pl.pallas_call(
            functools.partial(body, sizes),
            out_shape=V(*vort.shape),
            in_specs=[pl.BlockSpec(memory_space=pl.ANY)] * 2,
            out_specs=pl.BlockSpec(memory_space=pltpu.VMEM),
            scratch_shapes=[
                V(3, X, Y, Z), V(3, X, Y, Z),
                V(3, 5, X, Y, Z), V(4, X, 2, Z), V(3, 3, X, Y, Z), V(3, X, Y, Z),
                V(12, Y + 8, Z), V(6, 2, Y + 8, Z), V(3, 5, 2, Y + 8, Z), V(3, 3, 2, Y + 8, Z),
                V(S, 2, 3, 2, Y, Z), V(S, 2, 3, 2, Y, Z),
                V(S, 2, 3, X, 2, Z), V(S, 2, 3, X, 2, Z),
                V(S, 2, 2, 3, 2, 2, Z), V(S, 2, 2, 3, 2, 2, Z),
                V(2, 3, 2, Y, Z),
                V(2, 3, X, 2, Z), V(2, 3, X, 2, Z),
                V(2, 2, Y, Z), V(2, 2, Y, Z),
                V(2, 3, Y, Z), V(2, 3, Y, Z),
                V(2, 12, 4, Z), V(2, 12, 4, Z),
                V(2, 2, 3, 4, Z), V(2, 2, 3, 4, Z),
                V(46 * Y + 36 * X + 240, 1, Z),
                pltpu.SemaphoreType.DMA((1,)),
                pltpu.SemaphoreType.DMA((GROUPS,)),
                pltpu.SemaphoreType.DMA((2,)),
                pltpu.SemaphoreType.REGULAR,
            ],
            compiler_params=pltpu.CompilerParams(collective_id=0, has_side_effects=True),
        )(vort, vel)

    placed = P(None, *AXES)
    return jax.shard_map(
        local, mesh=mesh, in_specs=(placed, placed), out_specs=placed, check_vma=False
    )
```

```python
import functools
import math

import jax
import jax.numpy as jnp
from jax import lax
from jax.experimental import pallas as pl
from jax.experimental.pallas import tpu as pltpu
from jax.sharding import PartitionSpec as P

SUBSTEPS = 2
TIME_STEP = 0.5
AXES = ("gx", "gy", "gz")
MESH = pl.DeviceIdType.MESH
SIDES = (-1, 1)
GROUPS = 14


def roll(values, shift, axis):
    shift %= values.shape[axis]
    return pltpu.roll(values, shift, axis) if shift else values


def weights(velocity):
    d = TIME_STEP * velocity
    s = jnp.abs(d)
    t = 1.0 - s
    positive = d > 0.0
    centre = 1.0 + s * s * (1.5 * s - 2.5)
    toward = 1.0 + t * t * (1.5 * t - 2.5)
    away = -0.5 * s * t * t
    beyond = -0.5 * s * s * t
    return (
        jnp.where(positive, 0.0, beyond),
        jnp.where(positive, away, toward),
        centre,
        jnp.where(positive, toward, away),
        jnp.where(positive, beyond, 0.0),
    )


def inside(w, a, index, extent):
    if a == 0:
        return w
    return jnp.where(index < extent - a if a > 0 else index >= -a, w, 0.0)


def body(
    sizes, vort_hbm, vel_hbm, out, vort, vel, wgt, wgt_y, slope, cur,
    ext, pair, wgt_s, slope_s,
    sx, rx, sy, ry, sxy, rxy, rvx, svy, rvy, sz, rz, ssx, rsx, ssy, rsy, ssxy, rsxy,
    total, send_sem, recv_sem, load_sem, ready,
):
    _, X, Y, Z = vort.shape
    W = 8
    H = 4 * W
    assert (X + 8) * W == Z and 2 * H + X * W == Z and Y >= 8
    scale = TIME_STEP / 12.0
    here = [lax.axis_index(a) for a in AXES]

    def device(*offset):
        return tuple(
            here[k] if not d else lax.rem(here[k] + (d % sizes[k]), sizes[k])
            for k, d in enumerate(offset)
        )

    rows = {}

    def push(src, dst, offset, group, start=True):
        rows.setdefault(group, 0)
        rows[group] += math.prod(src.shape[:-1])
        copy = pltpu.make_async_remote_copy(
            src_ref=src, dst_ref=dst, send_sem=send_sem.at[0],
            recv_sem=recv_sem.at[list(rows).index(group)],
            device_id=device(*offset), device_id_type=MESH,
        )
        if start:
            copy.start()
        return copy

    def tally(n, group=0):
        some = total.at[pl.ds(0, n)]
        return pltpu.make_async_remote_copy(
            src_ref=some, dst_ref=some, send_sem=send_sem.at[0], recv_sem=recv_sem.at[group],
            device_id=device(1, 0, 0), device_id_type=MESH,
        )

    def arrived(group):
        tally(rows[group], list(rows).index(group)).wait_recv()

    loads = [
        pltpu.make_async_copy(vel_hbm, vel, load_sem.at[0]),
        pltpu.make_async_copy(vort_hbm, vort, load_sem.at[1]),
    ]
    for cp in loads:
        cp.start()

    plane = [(dx, dy, 0) for dx in (-1, 0, 1) for dy in (-1, 0, 1) if dx or dy]
    bottom, top = here[2] == 0, here[2] == sizes[2] - 1
    barrier = pltpu.get_barrier_semaphore()

    def greet(offset):
        pl.semaphore_signal(barrier, inc=1, device_id=device(*offset), device_id_type=MESH)

    for offset in plane:
        greet(offset)
    greet((0, 0, -1))

    @pl.when(jnp.logical_not(top))
    def _():
        greet((0, 0, 1))

    wide = lax.broadcasted_iota(jnp.int32, (Y + 8, Z), 1)
    lane = lax.broadcasted_iota(jnp.int32, (Y, Z), 1)
    row = lax.broadcasted_iota(jnp.int32, (Y, Z), 0)
    cell = lane % W
    edge = (lane < 2) | (lane >= Z - 2)
    rim = (lane < 4) | (lane >= Z - 4)

    def faces(src, c):
        found = roll(src[c, 0], H + 4, 1)
        for x in range(1, X):
            found = jnp.where(lane >= H + W * x, roll(src[c, x], H + W * x + 4, 1), found)
        return found

    def spread_x(src, step, s, components=range(3)):
        for c in components:
            if s == 0:
                sx[step, 0, c, 0] = wgt[0, 0, 0] * src[c, 0]
                sx[step, 0, c, 1] = wgt[0, 1, 0] * src[c, 0] + wgt[0, 0, 1] * src[c, 1]
            else:
                sx[step, 1, c, 0] = (
                    wgt[0, 3, X - 1] * src[c, X - 1] + wgt[0, 4, X - 2] * src[c, X - 2])
                sx[step, 1, c, 1] = wgt[0, 4, X - 1] * src[c, X - 1]
            for t in range(2):
                sxy[step, s, t, c] = sx[step, s, c, :, pl.ds((Y - 2) * t, 2), :]

    def push_x(step, s, group, part=slice(None)):
        def piece(ref):
            return ref if part == slice(None) else ref.at[part]

        push(piece(sx.at[step, s]), piece(rx.at[step, s]), (SIDES[s], 0, 0), group)
        for t in range(2):
            push(
                piece(sxy.at[step, s, t]), piece(rxy.at[step, s, t]), (SIDES[s], SIDES[t], 0),
                group)

    def offer(first, values):
        for i, v in enumerate(values, first):
            ext[i, pl.ds(4, Y)] = v
            for t in range(2):
                ssy[t, i] = v[(Y - 4) * t:(Y - 4) * t + 4]

    def bundle(m):
        for s in range(2):
            found = None
            for j in range(4):
                moved = roll(ext[4 * m + j, pl.ds(4, Y)], H * (j - 1 - s), 1)
                found = moved if found is None else jnp.where(lane >= H * j, moved, found)
            ssx[s, m] = found
            for t in range(2):
                ssxy[s, t, m] = found[(Y - 4) * t:(Y - 4) * t + 4]

    def push_strip(bundles, units):
        for s in (1, 0):
            push(ssx.at[s, bundles], rsx.at[s, bundles], (SIDES[s], 0, 0), "strip")
            for t in range(2):
                push(
                    ssxy.at[s, t, bundles], rsxy.at[s, t, bundles], (SIDES[s], SIDES[t], 0),
                    "strip")
        for t in range(2):
            push(ssy.at[t, units], rsy.at[t, units], (0, SIDES[t], 0), "strip")

    def interior_x(src, step):
        for c in range(3):
            layers = []
            for x in range(X):
                total = None
                for a in range(-2, 3):
                    if 0 <= x - a < X:
                        term = wgt[0, a + 2, x - a] * src[c, x - a]
                        total = term if total is None else total + term
                layers.append(total)
            for x in range(X):
                cur[c, x] = layers[x]
                for t in range(2):
                    sy[step, t, c, x] = layers[x][(Y - 2) * t:(Y - 2) * t + 2]

    def push_y(step):
        for t in range(2):
            push(sy.at[step, t], ry.at[step, t], (0, SIDES[t], 0), f"y{step}")

    def put_weights(k, layers):
        for x in layers:
            for a, w in enumerate(weights(vel[k, x])):
                if k == 1:
                    w = inside(w, a - 2, row, Y)
                if k == 2:
                    w = inside(w, a - 2, lane, Z)
                wgt[k, a, x] = w

    def ends(total, low, high, w):
        near = w[0] * low
        first = w[1] * low + jnp.concatenate([near[1:2], jnp.zeros_like(near[:1])], 0)
        near = w[2] * high
        last = w[3] * high + jnp.concatenate([jnp.zeros_like(near[:1]), near[0:1]], 0)
        gap = jnp.zeros((Y - 4, Z), jnp.float32)
        return total + jnp.concatenate([first, gap, last], 0)

    def pass_yz(step, x, components=range(3)):
        after = []
        for c in components:
            v = cur[c, x]
            low, high = ry[step, 1, c, x], ry[step, 0, c, x]
            for s, i in ((1, x), (0, x - X + 2)):
                if 0 <= i < 2:
                    v = v + rx[step, s, c, i]
                    low = low + rxy[step, s, 1, c, i]
                    high = high + rxy[step, s, 0, c, i]
            total = wgt[1, 2, x] * v
            for a in (-2, -1, 1, 2):
                total = total + roll(wgt[1, a + 2, x] * v, a, 0)
            v = ends(total, low, high, [wgt_y[i, x] for i in range(4)])
            if step > 0:
                v = jnp.where(edge, 0.0, v)
            total = wgt[2, 2, x] * v
            for a in (-2, -1, 1, 2):
                total = total + roll(wgt[2, a + 2, x] * v, a, 1)
            after.append(total)
        return after

    def stretch(v, steepness):
        total = []
        for i in range(3):
            t = v[i]
            for j in range(3):
                t = t + v[j] * steepness(j, i)
            total.append(t)
        return total

    def passes(values, w, axes):
        for k, axis, size in axes:
            total = w(k, 2) * values
            for a in (-2, -1, 1, 2):
                total = total + roll(w(k, a + 2) * values, size * a, axis)
            values = total
        return values

    def slope_rows(v, axis, n=1):
        near = roll(v, -n, axis) - roll(v, n, axis)
        return scale * (8.0 * near - (roll(v, -2 * n, axis) - roll(v, 2 * n, axis)))

    def slope_ends(dst, v, low, high):
        top, end = v[0:4], v[Y - 4:Y]
        dst[0:1] = scale * (8.0 * (top[1:2] - low[1:2]) - (top[2:3] - low[0:1]))
        dst[1:2] = scale * (8.0 * (top[2:3] - top[0:1]) - (top[3:4] - low[1:2]))
        dst[Y - 2:Y - 1] = scale * (8.0 * (end[3:4] - end[1:2]) - (high[0:1] - end[0:1]))
        dst[Y - 1:Y] = scale * (8.0 * (high[0:1] - end[2:3]) - (high[1:2] - end[1:2]))

    def slope_x(layers, components=range(3)):
        for c in components:
            def layer(x):
                if x < 0:
                    return rvx[1, c, x + 2]
                if x >= X:
                    return rvx[0, c, x - X]
                return vel[c, x]
            for x in layers:
                slope[0, c, x] = scale * (
                    8.0 * (layer(x + 1) - layer(x - 1)) - (layer(x + 2) - layer(x - 2)))

    loads[0].wait()
    put_weights(0, [0, 1, X - 2, X - 1])
    loads[1].wait()
    for s in (1, 0):
        spread_x(vort, 0, s)
    own = [faces(vort, c) for c in range(3)] + [faces(vel, c) for c in range(3)]
    middle = (lane >= H) & (lane < Z - H)
    for m in range(2):
        for up in range(2):
            found = None
            for j, v in enumerate(own[4 * m:4 * m + 4]):
                h, late = j % 2, j // 2
                moved = roll(v, 2 * H * h + 4 * (late - 1 + up), 1)
                spot = middle == (h == 0)
                if late:
                    spot = spot & (cell >= 4)
                found = moved if found is None else jnp.where(spot, moved, found)
            sz[up, m] = found
    pl.semaphore_wait(barrier, len(plane) + 1 + jnp.where(bottom, 0, 1))

    @pl.when(top)
    def _():
        pl.semaphore_signal(ready, inc=1, device_id=device(0, 0, 1), device_id_type=MESH)

    push(sz.at[1], rz.at[1], (0, 0, 1), "z")
    z_down = push(sz.at[0], rz.at[0], (0, 0, -1), "z", start=False)

    @pl.when(jnp.logical_not(bottom))
    def _():
        z_down.start()

    for s in (1, 0):
        push_x(0, s, f"x{s}")
        near = pl.ds((X - 2) * s, 2)
        if s:
            push(vel.at[:, near], rvx.at[s], (SIDES[s], 0, 0), "x1")
        else:
            for c in range(3):
                push(vel.at[c, near], rvx.at[s, c], (SIDES[s], 0, 0), f"vel{c}")
    for t in range(2):
        svy[t] = vel[:, :, pl.ds((Y - 2) * t, 2), :]
        push(svy.at[t], rvy.at[t], (0, SIDES[t], 0), "vel_y")
    put_weights(0, range(2, X - 2))
    interior_x(vort, 0)
    push_y(0)
    offer(0, own)
    bundle(0)
    push_strip(pl.ds(0, 1), pl.ds(0, 6))
    put_weights(1, range(X))
    put_weights(2, range(X))
    for c in range(3):
        for x in range(X):
            slope[1, c, x] = slope_rows(vel[c, x], 0)
            slope[2, c, x] = slope_rows(vel[c, x], 1)
    slope_x(range(2, X - 2))
    arrived("vel_y")
    for x in range(X):
        low, high = weights(rvy[1, 1, x]), weights(rvy[0, 1, x])
        for i, w in enumerate((low[3], low[4], high[1], high[0])):
            wgt_y[i, x] = w
    for c in range(3):
        for x in range(X):
            slope_ends(slope.at[1, c, x], vel[c, x], rvy[1, c, x], rvy[0, c, x])

    @pl.when(bottom)
    def _():
        pl.semaphore_wait(ready, 1)
        z_down.start()

    def advance(layers):
        for x in layers:
            v = stretch(pass_yz(0, x), lambda j, i: slope[j, i, x])
            for c in range(3):
                cur[c, x] = v[c]

    arrived("z")
    beyond = []
    for i in range(6):
        h, late = i % 2, i % 4 // 2
        below = roll(rz[1, i // 4], 2 * H * h - 4 * late, 1)
        above = roll(rz[0, i // 4], 2 * H * h + 4 - 4 * late, 1)
        beyond.append(jnp.where(cell < 4, below, above))
    offer(6, beyond)
    bundle(1)
    bundle(2)
    push_strip(pl.ds(1, 2), pl.ds(6, 6))

    arrived("y0")
    advance(range(2, X - 2))
    arrived("x1")
    slope_x([0, 1])
    advance([0, 1])
    spread_x(cur, 1, 0)
    push_x(1, 0, "x0 again")

    arrived("x0")
    rest, along = {}, {}
    for x in (X - 2, X - 1):
        v = pass_yz(0, x)
        along[x] = v[0]
        rest[x] = [v[i] + v[1] * slope[1, i, x] + v[2] * slope[2, i, x] for i in range(3)]
    for c in range(3):
        arrived(f"vel{c}")
        slope_x([X - 2, X - 1], [c])
        for x in (X - 2, X - 1):
            cur[c, x] = rest[x][c] + along[x] * slope[0, c, x]
        spread_x(cur, 1, 1, [c])
        push_x(1, 1, f"x1 again{c}", c)
    interior_x(cur, 1)
    push_y(1)

    for c in range(3):
        mine, other = ext[3 + c, pl.ds(4, Y)], ext[9 + c, pl.ds(4, Y)]
        left = slope_rows(jnp.where(cell < 4, other, mine), 1)
        right = slope_rows(jnp.where(cell < 4, mine, other), 1)
        steep = jnp.where(cell >= 4, left, right)
        for x in range(X):
            slope[2, c, x] = jnp.where(edge, roll(steep, -(H + W * x + 4), 1), slope[2, c, x])

    arrived("strip")
    tip = lane[:8]
    for i in range(12):
        m, j = divmod(i, 4)
        below, above = roll(rsx[1, m], -H * j, 1), roll(rsx[0, m], -H * (j + 1), 1)
        v = ext[i, pl.ds(4, Y)]
        ext[i, pl.ds(4, Y)] = jnp.where(lane < H, below, jnp.where(lane >= Z - H, above, v))
        below, above = [
            roll(jnp.concatenate([rsxy[s, 1, m], rsxy[s, 0, m]], 0), -H * (j + 1 - s), 1)
            for s in (1, 0)
        ]
        v = jnp.concatenate([rsy[1, i], rsy[0, i]], 0)
        v = jnp.where(tip < H, below, jnp.where(tip >= Z - H, above, v))
        ext[i, pl.ds(0, 4)] = v[0:4]
        ext[i, pl.ds(Y + 4, 4)] = v[4:8]
    inner = wide % W
    held = (inner >= 2) & (inner < 6)
    for i in range(6):
        pair[i, 0] = jnp.where(inner < 4, ext[6 + i], ext[i])
        pair[i, 1] = jnp.where(inner < 4, ext[i], ext[6 + i])
    for k in range(3):
        for a, w in enumerate(weights(pair[3 + k])):
            wgt_s[k, a] = w
    for c in range(3):
        v = pair[3 + c]
        for k, (axis, n) in enumerate(((2, W), (1, 1), (2, 1))):
            slope_s[k, c] = slope_rows(v, axis, n)

    def w(k, a):
        return wgt_s[k, a]

    in_x, in_y, in_z = (0, 2, W), (1, 1, 1), (2, 2, 1)
    v = [passes(pair[c], w, (in_x, in_y, in_z)) for c in range(3)]
    v = stretch(v, lambda j, i: slope_s[j, i])
    v = [passes(u, w, (in_x, in_y)) for u in v]
    v = [passes(jnp.where(held, u, 0.0), w, (in_z,)) for u in v]
    reach = [jnp.where(cell >= 4, u[0, 4:Y + 4], u[1, 4:Y + 4]) for u in v]
    def settle(layers):
        for x in layers:
            v = [
                u + jnp.where(rim, roll(reach[c], -(H + W * x + 4), 1), 0.0)
                for c, u in enumerate(pass_yz(1, x))
            ]
            v = stretch(v, lambda j, i: slope[j, i, x])
            for c in range(3):
                out[c, x] = v[c]

    arrived("y1")
    settle(range(2, X - 2))
    arrived("x0 again")
    settle([X - 2, X - 1])
    late = {0: [], 1: []}
    for c in range(3):
        arrived(f"x1 again{c}")
        for x in (0, 1):
            late[x].append(
                pass_yz(1, x, [c])[0]
                + jnp.where(rim, roll(reach[c], -(H + W * x + 4), 1), 0.0))
    for x in (0, 1):
        v = stretch(late[x], lambda j, i: slope[j, i, x])
        for c in range(3):
            out[c, x] = v[c]
    assert len(rows) == GROUPS and sum(rows.values()) == total.shape[0]
    tally(sum(rows.values())).wait_send()


def solution(mesh):
    sizes = [mesh.shape[a] for a in AXES]

    def local(vort, vel):
        _, X, Y, Z = vort.shape
        S = SUBSTEPS

        def V(*shape):
            return pltpu.VMEM(shape, jnp.float32)

        return pl.pallas_call(
            functools.partial(body, sizes),
            out_shape=V(*vort.shape),
            in_specs=[pl.BlockSpec(memory_space=pl.ANY)] * 2,
            out_specs=pl.BlockSpec(memory_space=pltpu.VMEM),
            scratch_shapes=[
                V(3, X, Y, Z), V(3, X, Y, Z),
                V(3, 5, X, Y, Z), V(4, X, 2, Z), V(3, 3, X, Y, Z), V(3, X, Y, Z),
                V(12, Y + 8, Z), V(6, 2, Y + 8, Z), V(3, 5, 2, Y + 8, Z), V(3, 3, 2, Y + 8, Z),
                V(S, 2, 3, 2, Y, Z), V(S, 2, 3, 2, Y, Z),
                V(S, 2, 3, X, 2, Z), V(S, 2, 3, X, 2, Z),
                V(S, 2, 2, 3, 2, 2, Z), V(S, 2, 2, 3, 2, 2, Z),
                V(2, 3, 2, Y, Z),
                V(2, 3, X, 2, Z), V(2, 3, X, 2, Z),
                V(2, 2, Y, Z), V(2, 2, Y, Z),
                V(2, 3, Y, Z), V(2, 3, Y, Z),
                V(2, 12, 4, Z), V(2, 12, 4, Z),
                V(2, 2, 3, 4, Z), V(2, 2, 3, 4, Z),
                V(46 * Y + 36 * X + 240, 1, Z),
                pltpu.SemaphoreType.DMA((1,)),
                pltpu.SemaphoreType.DMA((GROUPS,)),
                pltpu.SemaphoreType.DMA((2,)),
                pltpu.SemaphoreType.REGULAR,
            ],
            compiler_params=pltpu.CompilerParams(collective_id=0, has_side_effects=True),
        )(vort, vel)

    placed = P(None, *AXES)
    return jax.shard_map(
        local, mesh=mesh, in_specs=(placed, placed), out_specs=placed, check_vma=False
    )
```
